256 devices in a mesh: row: 32 (over x_hi, z, core), col: 8 (over y, x_lo).
Axes of the slice: x: 4 (x_hi: 2, x_lo: 2; x = x_hi * 2 + x_lo), y: 4, z: 8, core: 2. Of those that a mesh axis runs over, the one named last changes fastest.
Arguments:
- seq_state: bfloat16 [2048, 1024], P('row'), may hold values from -6 to 6
- pair_state: bfloat16 [2048, 2048, 128], P('row', 'col'), may hold values from -8 to 8
- w_bias: bfloat16 [128, 32], replicated, may hold values from -12 to 12
- w_qkv: bfloat16 [3, 1024, 1024], P(None, None, 'col'), may hold values from -0.1875 to 0.1875
- w_gate: bfloat16 [1024, 1024], P(None, 'col'), may hold values from -0.1875 to 0.1875
- w_out: bfloat16 [1024, 1024], replicated, may hold values from -0.8984375 to 0.8984375
- w_seq_pair: bfloat16 [1024, 128], replicated, may hold values from -0.1875 to 0.1875
- w_pair_out: bfloat16 [128, 128], replicated, may hold values from -0.5 to 0.5
- w_up: bfloat16 [128, 512], replicated, may hold values from -0.5 to 0.5
- w_down: bfloat16 [512, 128], replicated, may hold values from -0.25 to 0.25
Outputs:
- seq_out: bfloat16 [2048, 1024], P('row')
- pair_out: bfloat16 [2048, 2048, 128], P('row', 'col')
The draws below stay inside these ranges and needn't reach their ends.
All inputs are finite; a program needn't handle non-finite values.
Results may differ from the reference program's by a relative error of at most 0.018.
The reference program's roundings to bfloat16 on the way count: a program that leaves them out, or rounds other values in their place, can miss the bound.
Values may be sent and summed in bfloat16 or wider, within the bound.
A program may use at most 64 MiB of HBM per device.

```python
import math
import jax
import jax.numpy as jnp
from jax import lax

RES_DEV = 64
L = 2048
D = 1024
H = 32
P_SIZE = 128
INNER = 64
HID = 512


def draw_w_bias(key, part):
    base_draw = jnp.clip(jax.random.normal(jax.random.fold_in(key, 11), (P_SIZE, H), jnp.float32), -5.0, 5.0) * (2.0 / math.sqrt(P_SIZE))
    return base_draw.astype(jnp.bfloat16)


def draw_pair_state(key, part):
    values = jnp.clip(jax.random.normal(jax.random.fold_in(key, 23), (L, L, P_SIZE), jnp.float32), -6.0, 6.0)
    return values.astype(jnp.bfloat16)


def level_of(stream_key, extent, pieces, smallest, top_value):
    def one(axis_at, blocks):
        draws = jax.random.uniform(jax.random.fold_in(jax.random.fold_in(stream_key, 6), axis_at), (blocks,), jnp.float32, smallest / len(pieces), top_value / len(pieces))
        return jnp.repeat(jnp.exp(draws), extent[axis_at] // blocks).reshape((-1,) + (1,) * (len(extent) - axis_at - 1))

    level = one(*pieces[0])
    for cut in pieces[1:]:
        level = level * one(*cut)
    return level


def gaussian(key, dims, deviation, most, split=(), held_as=jnp.bfloat16):
    factor_of = level_of(key, dims, split, -0.22, 0.18) if split else 1.0
    values = jax.random.normal(key, dims, jnp.float32) * deviation * factor_of
    return jnp.minimum(jnp.maximum(values, -most), most).astype(held_as)


def setup_inputs(seed: int = 0) -> dict:
    arg_keys = jax.random.split(jax.random.key(seed), 11)
    seq_state = gaussian(arg_keys[0], (L, D), 1.0, 6.0, ((0, 32),))
    pair_state = draw_pair_state(jax.random.fold_in(arg_keys[10], 71), 0)
    w_bias = draw_w_bias(jax.random.fold_in(arg_keys[10], 71), 0)
    w_qkv = gaussian(arg_keys[3], (3, D, D), D ** -0.5, 0.1875, ((2, 8),))
    w_gate = gaussian(arg_keys[4], (D, D), D ** -0.5, 0.1875, ((1, 8),))
    w_out = gaussian(arg_keys[5], (D, D), 0.15, 0.8984375)
    w_seq_pair = gaussian(arg_keys[6], (D, 2 * INNER), D ** -0.5, 0.1875)
    w_pair_out = gaussian(arg_keys[7], (2 * INNER, P_SIZE), (2 * INNER) ** -0.5, 0.5)
    w_up = gaussian(arg_keys[8], (P_SIZE, HID), P_SIZE ** -0.5, 0.5)
    w_down = gaussian(arg_keys[9], (HID, P_SIZE), HID ** -0.5, 0.25)
    return dict(seq_state=seq_state, pair_state=pair_state, w_bias=w_bias, w_qkv=w_qkv, w_gate=w_gate, w_out=w_out, w_seq_pair=w_seq_pair, w_pair_out=w_pair_out, w_up=w_up, w_down=w_down)


EPSILON = 1e-05

def layer_norm(values):
    centred = values - lax.optimization_barrier(jnp.mean(values, axis=-1, keepdims=True))
    variance = lax.optimization_barrier(jnp.mean(centred * centred, axis=-1, keepdims=True))
    return centred * lax.rsqrt(variance + EPSILON)

def reference(seq_state, pair_state, w_bias, w_qkv, w_gate, w_out, w_seq_pair, w_pair_out, w_up, w_down):
    length = seq_state.shape[0]
    model_width = seq_state.shape[1]
    head_count = w_bias.shape[1]
    head_size = model_width // head_count
    channels = pair_state.shape[2]
    blocks = length // RES_DEV
    normed = layer_norm(seq_state.astype(jnp.float32)).astype(jnp.bfloat16)
    queries = jnp.dot(normed, w_qkv[0], preferred_element_type=jnp.float32).astype(jnp.bfloat16)
    keys_all = jnp.dot(normed, w_qkv[1], preferred_element_type=jnp.float32).astype(jnp.bfloat16)
    values_all = jnp.dot(normed, w_qkv[2], preferred_element_type=jnp.float32).astype(jnp.bfloat16)
    gate_values = jax.nn.sigmoid(jnp.dot(normed, w_gate, preferred_element_type=jnp.float32))

    def bias_block(block_rows):
        pair_normed = layer_norm(block_rows.astype(jnp.float32)).astype(jnp.bfloat16)
        flat_norm = pair_normed.reshape(-1, channels)
        return jnp.dot(flat_norm, w_bias, preferred_element_type=jnp.float32).astype(jnp.bfloat16).reshape(block_rows.shape[0], length, head_count)
    bias = lax.map(bias_block, pair_state.reshape(blocks, RES_DEV, length, channels)).reshape(length, length, head_count)
    scale = 1.0 / math.sqrt(head_size)

    def one_head(head_index):
        first_col = head_index * head_size
        query_head = lax.dynamic_slice_in_dim(queries, first_col, head_size, 1)
        key_head = lax.dynamic_slice_in_dim(keys_all, first_col, head_size, 1)
        value_head = lax.dynamic_slice_in_dim(values_all, first_col, head_size, 1)
        head_bias = lax.dynamic_index_in_dim(bias, head_index, 2, keepdims=False)
        scores = jnp.dot(query_head, key_head.T, preferred_element_type=jnp.float32) * scale + head_bias.astype(jnp.float32)
        row_peak = lax.optimization_barrier(jnp.max(scores, axis=-1, keepdims=True))
        weights = jnp.exp(scores - row_peak)
        probs = (weights / lax.optimization_barrier(jnp.sum(weights, axis=-1, keepdims=True))).astype(jnp.bfloat16)
        return jnp.dot(probs, value_head, preferred_element_type=jnp.float32)
    heads_out = lax.map(one_head, jnp.arange(head_count, dtype=jnp.int32))
    mixed_heads = jnp.transpose(heads_out, (1, 0, 2)).reshape(length, model_width)
    attended = (mixed_heads * gate_values).astype(jnp.bfloat16)
    update_seq = jnp.dot(attended, w_out, preferred_element_type=jnp.float32)
    seq_out = (seq_state.astype(jnp.float32) + update_seq).astype(jnp.bfloat16)
    new_normed = layer_norm(seq_out.astype(jnp.float32)).astype(jnp.bfloat16)
    inner_width = w_seq_pair.shape[1] // 2
    projected = lax.optimization_barrier(jnp.dot(new_normed, w_seq_pair, preferred_element_type=jnp.float32).astype(jnp.bfloat16))
    left_side = projected[:, :inner_width].astype(jnp.float32)
    right_side = projected[:, inner_width:].astype(jnp.float32)

    def pair_block(block_items):
        block_rows, left_rows = block_items
        product = left_rows[:, None, :] * right_side[None, :, :]
        difference = left_rows[:, None, :] - right_side[None, :, :]
        features = jnp.concatenate([product, difference], axis=-1).astype(jnp.bfloat16).reshape(-1, 2 * inner_width)
        updated = block_rows.astype(jnp.float32).reshape(-1, channels) + jnp.dot(features, w_pair_out, preferred_element_type=jnp.float32)
        hidden = jax.nn.relu(jnp.dot(layer_norm(updated).astype(jnp.bfloat16), w_up, preferred_element_type=jnp.float32)).astype(jnp.bfloat16)
        result = updated + jnp.dot(hidden, w_down, preferred_element_type=jnp.float32)
        return result.astype(jnp.bfloat16).reshape(block_rows.shape)
    pair_out = lax.map(pair_block, (pair_state.reshape(blocks, RES_DEV, length, channels), left_side.reshape(blocks, RES_DEV, inner_width)))
    return (seq_out, pair_out.reshape(length, length, channels))
```

```python
import math

import jax
import jax.numpy as jnp
from jax import lax
from jax.experimental import pallas as pl
from jax.experimental.pallas import tpu as pltpu
from jax.sharding import PartitionSpec as P

EPSILON = 1e-05

F32 = jnp.float32
BF16 = jnp.bfloat16
PAIR_ROWS = 16
PAIR_CHUNK = 4


def dot32(a, b):
    return jnp.dot(a, b, preferred_element_type=F32)


def pair_kernel(x_ref, left_ref, right_ref, wp_ref, wu_ref, wd_ref, o_ref, mix_ref, right2_ref):
    @pl.when(pl.program_id(0) == 0)
    def _():
        w = wp_ref[...].astype(F32)
        centred = w - jnp.mean(w, axis=1, keepdims=True)
        a = lax.broadcasted_iota(jnp.int32, (128, 128), 0)
        b = lax.broadcasted_iota(jnp.int32, (128, 128), 1)
        eye = jnp.where(a == b, 1.0, 0.0)
        mix_ref[0:128, 0:128] = (eye - 1.0 / 128).astype(BF16)
        mix_ref[0:128, 128:256] = eye.astype(BF16)
        mix_ref[128:256, 0:128] = centred.astype(BF16)
        mix_ref[128:256, 128:256] = wp_ref[...]
        r = right_ref[...].astype(F32)
        right2_ref[...] = jnp.concatenate([r, r], axis=1)

    lane = lax.broadcasted_iota(jnp.int32, (1, 128), 1)
    for start in range(0, PAIR_ROWS, PAIR_CHUNK):
        features, rows = [], []
        for i in range(start, start + PAIR_CHUNK):
            left = left_ref[pl.ds(i, 1), :].astype(F32)
            left2 = jnp.concatenate([left, left], axis=1)
            scale = jnp.where(lane < 64, left2, -1.0)
            shift = jnp.where(lane < 64, 0.0, left2)
            features.append((right2_ref[...] * scale + shift).astype(BF16))
            rows.append(x_ref[i])
        mixed = dot32(
            jnp.concatenate([jnp.concatenate(rows, axis=0), jnp.concatenate(features, axis=0)], axis=1),
            mix_ref[...],
        )
        centred, updated = mixed[:, :128], mixed[:, 128:]
        variance = jnp.mean(centred * centred, axis=1, keepdims=True)
        normed = (centred * lax.rsqrt(variance + EPSILON)).astype(BF16)
        hidden = jnp.maximum(dot32(normed, wu_ref[...]), 0.0).astype(BF16)
        result = (updated + dot32(hidden, wd_ref[...])).astype(BF16)
        for i in range(PAIR_CHUNK):
            o_ref[start + i] = result[i * 256 : (i + 1) * 256]


def pair_transition(x, left, right, wp, wu, wd):
    rows = x.shape[0]

    def whole(array):
        return pl.BlockSpec(array.shape, lambda i: (0,) * array.ndim)

    return pl.pallas_call(
        pair_kernel,
        grid=(rows // PAIR_ROWS,),
        out_shape=jax.ShapeDtypeStruct(x.shape, BF16),
        in_specs=[
            pl.BlockSpec((PAIR_ROWS, 256, 128), lambda i: (i, 0, 0)),
            pl.BlockSpec((PAIR_ROWS, 64), lambda i: (i, 0)),
            whole(right),
            whole(wp),
            whole(wu),
            whole(wd),
        ],
        out_specs=pl.BlockSpec((PAIR_ROWS, 256, 128), lambda i: (i, 0, 0)),
        scratch_shapes=[pltpu.VMEM((256, 256), BF16), pltpu.VMEM((256, 128), F32)],
        compiler_params=pltpu.CompilerParams(dimension_semantics=("arbitrary",)),
    )(x, left, right, wp, wu, wd)


def sent_to_all(x, axis):
    peers = lax.axis_size(axis)
    return lax.all_to_all(jnp.broadcast_to(x[None], (peers, *x.shape)), axis, 0, 0, tiled=True)


def laid_out(pieces, dim):
    pieces = jnp.moveaxis(pieces, 0, dim)
    lengths = pieces.shape
    return pieces.reshape(*lengths[:dim], lengths[dim] * lengths[dim + 1], *lengths[dim + 2 :])


def collect(x, axis, dim):
    pieces = sent_to_all(x, axis)
    return laid_out(pieces, dim)


def layer_norm(values):
    centred = values - jnp.mean(values, axis=-1, keepdims=True)
    variance = jnp.mean(centred * centred, axis=-1, keepdims=True)
    return centred * lax.rsqrt(variance + EPSILON)


def body(seq_state, pair_state, w_bias, w_qkv, w_gate, w_out, w_seq_pair, w_pair_out, w_up, w_down):
    rows_here, model_width = seq_state.shape
    cols_here = pair_state.shape[1]
    channels = pair_state.shape[2]
    head_count = w_bias.shape[1]
    local_width = w_gate.shape[1]
    head_size = model_width // head_count
    local_heads = local_width // head_size
    pair_normed = layer_norm(pair_state.astype(jnp.float32)).astype(jnp.bfloat16)
    bias_local = jnp.einsum(
        "rcp,ph->hrc", pair_normed, w_bias, preferred_element_type=jnp.float32
    ).astype(jnp.bfloat16)
    bias_rows = lax.all_to_all(bias_local, "col", split_axis=0, concat_axis=2, tiled=True)
    normed = layer_norm(seq_state.astype(jnp.float32)).astype(jnp.bfloat16)
    queries = jnp.dot(normed, w_qkv[0], preferred_element_type=jnp.float32).astype(jnp.bfloat16)
    own_keys = jnp.dot(normed, w_qkv[1], preferred_element_type=jnp.float32).astype(jnp.bfloat16)
    own_values = jnp.dot(normed, w_qkv[2], preferred_element_type=jnp.float32).astype(jnp.bfloat16)
    key_value = collect(jnp.stack([own_keys, own_values]), "row", 1)
    length = key_value.shape[1]
    query_heads = queries.reshape(rows_here, local_heads, head_size)
    key_heads = key_value[0].reshape(length, local_heads, head_size)
    value_heads = key_value[1].reshape(length, local_heads, head_size)
    scale = 1.0 / math.sqrt(head_size)
    scores = jnp.einsum(
        "rhe,lhe->hrl", query_heads, key_heads, preferred_element_type=jnp.float32
    ) * scale + bias_rows.astype(jnp.float32)
    row_peak = jnp.max(scores, axis=-1, keepdims=True)
    weights = jnp.exp(scores - row_peak)
    probs = (weights / jnp.sum(weights, axis=-1, keepdims=True)).astype(jnp.bfloat16)
    mixed_heads = jnp.einsum(
        "hrl,lhe->rhe", probs, value_heads, preferred_element_type=jnp.float32
    ).reshape(rows_here, local_width)
    gate_values = jax.nn.sigmoid(jnp.dot(normed, w_gate, preferred_element_type=jnp.float32))
    attended = (mixed_heads * gate_values).astype(jnp.bfloat16)
    gathered = collect(attended, "col", 1)
    update_seq = jnp.dot(gathered, w_out, preferred_element_type=jnp.float32)
    seq_out = (seq_state.astype(jnp.float32) + update_seq).astype(jnp.bfloat16)
    new_normed = layer_norm(seq_out.astype(jnp.float32)).astype(jnp.bfloat16)
    inner_width = w_seq_pair.shape[1] // 2
    left_side = lax.optimization_barrier(
        jnp.dot(new_normed, w_seq_pair[:, :inner_width], preferred_element_type=jnp.float32).astype(
            jnp.bfloat16
        )
    )
    right_side = jnp.einsum(
        "rd,di->ir", new_normed, w_seq_pair[:, inner_width:], preferred_element_type=jnp.float32
    ).astype(jnp.bfloat16)
    right_all = collect(right_side, "row", 1)
    right_cols = (
        lax.dynamic_slice_in_dim(right_all, lax.axis_index("col") * cols_here, cols_here, 1)
        .T
    )
    pair_out = pair_transition(pair_state, left_side, right_cols, w_pair_out, w_up, w_down)
    return (seq_out, pair_out)


def solution(mesh):
    return jax.shard_map(
        body,
        mesh=mesh,
        in_specs=(
            P("row", None),
            P("row", "col", None),
            P(),
            P(None, None, "col"),
            P(None, "col"),
            P(),
            P(),
            P(),
            P(),
            P(),
        ),
        out_specs=(P("row", None), P("row", "col", None)),
        check_vma=False,
    )
```

```python
import functools
import math

import jax
import jax.numpy as jnp
from jax import lax
from jax.experimental import pallas as pl
from jax.experimental.pallas import tpu as pltpu
from jax.sharding import PartitionSpec as P

EPSILON = 1e-05
F32 = jnp.float32
BF16 = jnp.bfloat16
PAIR_ROWS = 16
PAIR_CHUNK = 4
SCALE = 1.0 / math.sqrt(32)
NT = (((1,), (1,)), ((), ()))
Z_ORDER = (0, 1, 7, 2, 6, 3, 5, 4)


def dot32(a, b):
    return jnp.dot(a, b, preferred_element_type=F32)


def dot_nt(a, b):
    return lax.dot_general(a, b, NT, preferred_element_type=F32)


def norm_rows(values):
    centred = values - jnp.mean(values, axis=-1, keepdims=True)
    variance = jnp.mean(centred * centred, axis=-1, keepdims=True)
    return centred * lax.rsqrt(variance + EPSILON)


def front_kernel(
    seq_hbm, pair_hbm, wbias_hbm, wqkv_hbm, wgate_hbm, wout_hbm, wsp_hbm,
    seq_out_ref, left_ref, right_ref,
    seq_v, pair_v, wbias_v, wqkv_v, wgate_v, wout_v, wsp_v,
    seq32, zbuf, qbuf, gsend, grecv, kv, bias_v, o32, osend, orecv, m_c, l_c, mlsend, mlrecv,
    lrsend, lbuf, rbuf, sosend, sobuf,
    in_sem, pair_sem,
    z_s, z_r, q_s, q_r, g_s, g_r, a_s, kv_r, d_s, o_s, o_r, ml_s, ml_r, l_s, l_r, r_s, r_r, so_s, so_r,
):
    row = lax.axis_index("row")
    col = lax.axis_index("col")
    core = lax.rem(row, 2)
    z = lax.rem(row // 2, 8)
    xh = row // 16
    partner = row + 1 - 2 * core
    own_plane = xh == col // 4
    own_right = row // 4 == col

    loads = [
        pltpu.make_async_copy(src, dst, in_sem.at[n])
        for n, (src, dst) in enumerate(
            ((seq_hbm, seq_v), (wqkv_hbm, wqkv_v), (wgate_hbm, wgate_v), (wbias_hbm, wbias_v),
             (wout_hbm, wout_v), (wsp_hbm, wsp_v))
        )
    ]
    for n in range(4):
        loads[n].start()

    barrier = pltpu.get_barrier_semaphore()

    def greet(r, c):
        pl.semaphore_signal(barrier, inc=1, device_id=(r, c), device_id_type=pl.DeviceIdType.MESH)

    def z_row(k):
        return xh * 16 + lax.rem(z + k, 8) * 2 + core

    for d in range(1, 8):
        greet(z_row(d), col)
        greet(row, lax.rem(col + d, 8))
    greet(partner, col)
    plane_row = (col // 4) * 16 + z * 2 + core
    for c in range(8):
        @pl.when(jnp.logical_not(jnp.logical_and(own_plane, col == c)))
        def _():
            greet(plane_row, c)

    @pl.loop(0, 32)
    def _(n):
        r, c = 4 * col + n // 8, lax.rem(n, 8)

        @pl.when(jnp.logical_not(jnp.logical_and(own_right, jnp.logical_and(row == r, col == c))))
        def _():
            greet(r, c)

    def pair_load(n):
        return pltpu.make_async_copy(pair_hbm.at[pl.ds(n * 8, 8)], pair_v.at[pl.ds(n * 8, 8)], pair_sem.at[n])

    for n in range(8):
        pair_load(n).start()
    for n in (4, 5):
        loads[n].start()

    lane = lax.broadcasted_iota(jnp.int32, (1, 128), 1)
    loads[0].wait()
    x = seq_v[...].astype(F32)
    seq32[...] = x
    normed = norm_rows(x).astype(BF16)
    loads[1].wait()
    zbuf[0, 0:64] = dot32(normed, wqkv_v[1]).astype(BF16)
    zbuf[0, 64:128] = dot32(normed, wqkv_v[2]).astype(BF16)
    qbuf[0] = dot32(normed, wqkv_v[0]).astype(BF16)

    pl.semaphore_wait(
        barrier, 15 + 8 - own_plane.astype(jnp.int32) + 32 - own_right.astype(jnp.int32)
    )

    def remote(src, dst, ss, rs, r, c):
        return pltpu.make_async_remote_copy(
            src_ref=src, dst_ref=dst, send_sem=ss, recv_sem=rs, device_id=(r, c),
            device_id_type=pl.DeviceIdType.MESH,
        )

    def z_copy(d):
        return remote(zbuf.at[0], zbuf.at[d], z_s.at[d], z_r.at[d], z_row(d), col)

    def col_copy(src, dst, ss, rs, d):
        return remote(src, dst, ss.at[d], rs.at[d], row, lax.rem(col + d, 8))

    def q_copy(d):
        return col_copy(qbuf.at[0], qbuf.at[d], q_s, q_r, d)

    def g_copy(d):
        return col_copy(gsend.at[lax.rem(col + d, 8)], grecv.at[d], g_s, g_r, d)

    for d in (4, 3, 5, 2, 6, 1, 7):
        z_copy(d).start()

    loads[2].wait()
    gate = jax.nn.sigmoid(dot32(normed, wgate_v[...]))
    gsend[...] = gate.reshape(8, 8, 128)

    loads[3].wait()
    wb = wbias_v[...].astype(F32)
    wb_t = jnp.concatenate([wb, jnp.zeros((128, 96), F32)], axis=1).T[0:32].astype(BF16)
    ia = lax.broadcasted_iota(jnp.int32, (128, 128), 0)
    ib = lax.broadcasted_iota(jnp.int32, (128, 128), 1)
    centre = (jnp.where(ia == ib, 1.0, 0.0) - 1.0 / 128).astype(BF16)

    def bias_row(i):
        ct = dot_nt(centre, pair_v[i])
        variance = jnp.mean(ct * ct, axis=0, keepdims=True)
        n = (ct * lax.rsqrt(variance + EPSILON)).astype(BF16)
        b = dot32(wb_t, n).astype(BF16).astype(F32)
        bias_v[0, pl.ds(i, 32, stride=64), :] = b[:, 0:128]
        bias_v[1, pl.ds(i, 32, stride=64), :] = b[:, 128:256]

    def plane_copy(d, k):
        source = lax.rem(z + 8 - d, 8)
        return remote(
            zbuf.at[d], kv.at[lax.rem(source, 2) * 2 + core, col], a_s.at[d, k],
            kv_r.at[lax.rem(source, 2) * 2 + core, col], k * 16 + z * 2 + core, xh * 4 + source // 2,
        )

    def to_self(d, k):
        source = lax.rem(z + 8 - d, 8)
        return jnp.logical_and(xh == k, col == xh * 4 + source // 2)

    for step, d in enumerate(Z_ORDER):
        if d:
            z_copy(d).wait_recv()
        for k in range(2):
            here = to_self(d, k)

            @pl.when(here)
            def _():
                kv[lax.rem(z + 8 - d, 2) * 2 + core, col] = zbuf[d]

            @pl.when(jnp.logical_not(here))
            def _():
                plane_copy(d, k).start()

        if step == 0:
            for e in (4, 3, 5, 2, 6, 1, 7):
                q_copy(e).start()
        if step == 1:
            for e in (4, 3, 5, 2, 6, 1, 7):
                g_copy(e).start()
        pair_load(step).wait()

        @pl.loop(0, 8)
        def _(n):
            bias_row(step * 8 + n)

    def kv_wait(q, c):
        return remote(kv.at[q, c], kv.at[q, c], d_s.at[0, 0], kv_r.at[q, c], partner, col)

    def core_copy(h, c):
        q = h * 2 + core
        return remote(kv.at[q, c], kv.at[q, c], d_s.at[h, c], kv_r.at[q, c], partner, col)

    for h in range(2):
        @pl.loop(0, 8)
        def _(c):
            @pl.when(jnp.logical_not(jnp.logical_and(own_plane, col == c)))
            def _():
                kv_wait(h * 2 + core, c).wait_recv()

            core_copy(h, c).start()

    for d in range(1, 8):
        q_copy(d).wait_recv()
    for h in range(2):
        @pl.loop(0, 8)
        def _(c):
            kv_wait(h * 2 + 1 - core, c).wait_recv()

    m_c[...] = jnp.zeros_like(m_c)
    l_c[...] = jnp.ones_like(l_c)
    head_of = lane // 32

    @pl.loop(0, 8)
    def _(d):
        g = lax.rem(col + 8 - d, 8)
        q = qbuf[d].astype(F32)
        q4 = jnp.concatenate([jnp.where(head_of == t, q, 0.0) for t in range(4)], axis=0).astype(BF16)
        blocks = [kv[b, g] for b in range(4)]
        keys = jnp.concatenate([b[0:64] for b in blocks], axis=0)
        values = jnp.concatenate([b[64:128] for b in blocks], axis=0)
        at = pl.ds(pl.multiple_of(g * 256, 256), 256)
        bias = jnp.concatenate([bias_v[0, at], bias_v[1, at]], axis=1)
        scores = dot_nt(q4, keys) * SCALE + bias
        peak = jnp.max(scores, axis=1, keepdims=True)
        weights = jnp.exp(scores - peak)
        total = jnp.sum(weights, axis=1, keepdims=True)
        o4 = dot32(weights.astype(BF16), values)
        out = jnp.zeros((64, 128), F32)
        m, l = m_c[...], l_c[...]
        for t in range(4):
            part = slice(t * 64, t * 64 + 64)
            out = jnp.where(head_of == t, o4[part], out)
            m = jnp.where(lane == g * 4 + t, peak[part], m)
            l = jnp.where(lane == g * 4 + t, total[part], l)
        m_c[...] = m
        l_c[...] = l
        o32[:, pl.ds(pl.multiple_of(g * 8, 8), 8), :] = out.reshape(8, 8, 128)

    osend[...] = o32[...].astype(BF16)
    mlsend[:, 0:8] = m_c[...].reshape(8, 8, 128)
    mlsend[:, 8:16] = l_c[...].reshape(8, 8, 128)

    def o_copy(d):
        return col_copy(osend.at[lax.rem(col + d, 8)], orecv.at[d], o_s, o_r, d)

    def ml_copy(d):
        return col_copy(mlsend.at[lax.rem(col + d, 8)], mlrecv.at[d], ml_s, ml_r, d)

    for d in (4, 3, 5, 2, 6, 1, 7):
        ml_copy(d).start()
        o_copy(d).start()
    orecv[0] = osend[col]
    mlrecv[0] = mlsend[col]
    grecv[0] = gsend[col]
    ea = lax.broadcasted_iota(jnp.int32, (128, 1024), 0)
    eb = lax.broadcasted_iota(jnp.int32, (128, 1024), 1)
    expand = jnp.where(ea == eb // 32, 1.0, 0.0).astype(BF16)
    for d in range(1, 8):
        g_copy(d).wait_recv()
        ml_copy(d).wait_recv()
        o_copy(d).wait_recv()

    peaks = [mlrecv[p, 0:8] for p in range(8)]
    top = functools.reduce(jnp.maximum, peaks)
    shares = [jnp.exp(v - top) for v in peaks]
    whole = functools.reduce(jnp.add, [s * mlrecv[p, 8:16] for p, s in enumerate(shares)])
    share = jnp.concatenate([s / whole for s in shares], axis=0)
    high = share.astype(BF16)
    low = (share - high.astype(F32)).astype(BF16)
    wide = dot32(high, expand) + dot32(low, expand)
    parts = []
    for g in range(8):
        tile = jnp.zeros((8, 128), F32)
        for p in range(8):
            tile = tile + wide[p * 8 : p * 8 + 8, g * 128 : g * 128 + 128] * orecv[p].astype(F32)[g * 8 : g * 8 + 8]
        parts.append(tile * grecv[lax.rem(col + 8 - g, 8)])
    attended = jnp.concatenate(parts, axis=1).astype(BF16)
    loads[4].wait()
    update = dot32(attended, wout_v[...])
    new_seq = (seq32[pl.ds(pl.multiple_of(col * 8, 8), 8), :] + update).astype(BF16).astype(F32)
    new_normed = norm_rows(new_seq).astype(BF16)
    loads[5].wait()
    sides = dot32(new_normed, wsp_v[...]).astype(BF16).astype(F32)
    lrsend[...] = sides

    def r_copy(n):
        return remote(lrsend, rbuf.at[lax.rem(row, 4), col], r_s.at[n], r_r.at[lax.rem(row, 4), col], n, row // 4)

    def l_copy(d):
        return remote(lrsend, lbuf.at[col], l_s.at[d], l_r.at[col], row, lax.rem(col + d, 8))

    def so_copy(d):
        return remote(sosend, sobuf.at[col], so_s.at[d], so_r.at[col], row, lax.rem(col + d, 8))

    def right_here(n):
        return jnp.logical_and(own_right, row == n)

    @pl.loop(0, 32)
    def _(n):
        @pl.when(jnp.logical_not(right_here(n)))
        def _():
            r_copy(n).start()

    for d in (4, 3, 5, 2, 6, 1, 7):
        l_copy(d).start()
    sosend[...] = jnp.concatenate([new_seq[:, g * 128 : g * 128 + 128] for g in range(8)], axis=0).astype(BF16)
    for d in (4, 3, 5, 2, 6, 1, 7):
        so_copy(d).start()
    lbuf[col] = sides
    sobuf[col] = sosend[...]

    @pl.when(own_right)
    def _():
        rbuf[lax.rem(row, 4), col] = sides

    for d in range(1, 8):
        z_copy(d).wait_send()
        q_copy(d).wait_send()
        g_copy(d).wait_send()
        ml_copy(d).wait_send()
        o_copy(d).wait_send()
    for d in range(8):
        for k in range(2):
            @pl.when(jnp.logical_not(to_self(d, k)))
            def _():
                plane_copy(d, k).wait_send()
    for h in range(2):
        @pl.loop(0, 8)
        def _(c):
            core_copy(h, c).wait_send()

    def col_wait(buf, ss, rs, d):
        source = lax.rem(col + 8 - d, 8)
        return remote(buf.at[source], buf.at[source], ss.at[d], rs.at[source], row, source)

    for d in range(1, 8):
        col_wait(lbuf, l_s, l_r, d).wait_recv()
        col_wait(sobuf, so_s, so_r, d).wait_recv()
    left_ref[...] = lbuf[...].reshape(64, 128)
    for c in range(8):
        block = sobuf[c].astype(F32)
        o32[c] = block
    seq_out_ref[...] = jnp.concatenate(
        [o32[:, g * 8 : g * 8 + 8, :].reshape(64, 128) for g in range(8)], axis=1
    ).astype(BF16)
    for q in range(4):
        @pl.loop(0, 8)
        def _(c):
            @pl.when(jnp.logical_not(jnp.logical_and(own_right, jnp.logical_and(lax.rem(row, 4) == q, col == c))))
            def _():
                remote(rbuf.at[q, c], rbuf.at[q, c], r_s.at[0], r_r.at[q, c], partner, col).wait_recv()

    right_ref[...] = rbuf[...].reshape(256, 128)
    for d in range(1, 8):
        l_copy(d).wait_send()
        so_copy(d).wait_send()

    @pl.loop(0, 32)
    def _(n):
        @pl.when(jnp.logical_not(right_here(n)))
        def _():
            r_copy(n).wait_send()


def front(seq_state, pair_state, w_bias, w_qkv, w_gate, w_out, w_seq_pair):
    any_spec = pl.BlockSpec(memory_space=pl.ANY)
    vmem_spec = pl.BlockSpec(memory_space=pltpu.VMEM)
    dma = pltpu.SemaphoreType.DMA
    return pl.pallas_call(
        front_kernel,
        out_shape=(
            jax.ShapeDtypeStruct((64, 1024), BF16),
            jax.ShapeDtypeStruct((64, 128), F32),
            jax.ShapeDtypeStruct((256, 128), F32),
        ),
        in_specs=[any_spec] * 7,
        out_specs=(vmem_spec,) * 3,
        scratch_shapes=[
            pltpu.VMEM((64, 1024), BF16),
            pltpu.VMEM((64, 256, 128), BF16),
            pltpu.VMEM((128, 32), BF16),
            pltpu.VMEM((3, 1024, 128), BF16),
            pltpu.VMEM((1024, 128), BF16),
            pltpu.VMEM((1024, 1024), BF16),
            pltpu.VMEM((1024, 128), BF16),
            pltpu.VMEM((64, 1024), F32),
            pltpu.VMEM((8, 128, 128), BF16),
            pltpu.VMEM((8, 64, 128), BF16),
            pltpu.VMEM((8, 8, 128), F32),
            pltpu.VMEM((8, 8, 128), F32),
            pltpu.VMEM((4, 8, 128, 128), BF16),
            pltpu.VMEM((2, 2048, 128), F32),
            pltpu.VMEM((8, 64, 128), F32),
            pltpu.VMEM((8, 64, 128), BF16),
            pltpu.VMEM((8, 64, 128), BF16),
            pltpu.VMEM((64, 128), F32),
            pltpu.VMEM((64, 128), F32),
            pltpu.VMEM((8, 16, 128), F32),
            pltpu.VMEM((8, 16, 128), F32),
            pltpu.VMEM((8, 128), F32),
            pltpu.VMEM((8, 8, 128), F32),
            pltpu.VMEM((4, 8, 8, 128), F32),
            pltpu.VMEM((64, 128), BF16),
            pltpu.VMEM((8, 64, 128), BF16),
            dma((6,)), dma((8,)),
            dma((8,)), dma((8,)), dma((8,)), dma((8,)), dma((8,)), dma((8,)),
            dma((8, 2)), dma((4, 8)), dma((2, 8)),
            dma((8,)), dma((8,)), dma((8,)), dma((8,)), dma((8,)), dma((8,)),
            dma((32,)), dma((4, 8)), dma((8,)), dma((8,)),
        ],
        compiler_params=pltpu.CompilerParams(
            collective_id=0, has_side_effects=True, vmem_limit_bytes=48 * 1024 * 1024
        ),
        cost_estimate=pl.CostEstimate(flops=3_000_000_000, bytes_accessed=8_000_000, transcendentals=600_000),
    )(seq_state, pair_state, w_bias, w_qkv, w_gate, w_out, w_seq_pair)


def pair_kernel(x_ref, left_ref, right_ref, wp_ref, wu_ref, wd_ref, o_ref, mix_ref, right2_ref):
    @pl.when(pl.program_id(0) == 0)
    def _():
        w = wp_ref[...].astype(F32)
        centred = w - jnp.mean(w, axis=1, keepdims=True)
        a = lax.broadcasted_iota(jnp.int32, (128, 128), 0)
        b = lax.broadcasted_iota(jnp.int32, (128, 128), 1)
        eye = jnp.where(a == b, 1.0, 0.0)
        mix_ref[0:128, 0:128] = (eye - 1.0 / 128).astype(BF16)
        mix_ref[0:128, 128:256] = eye.astype(BF16)
        mix_ref[128:256, 0:128] = centred.astype(BF16)
        mix_ref[128:256, 128:256] = wp_ref[...]
        r = right_ref[:, 64:128]
        right2_ref[...] = jnp.concatenate([r, r], axis=1)

    lane = lax.broadcasted_iota(jnp.int32, (1, 128), 1)
    for start in range(0, PAIR_ROWS, PAIR_CHUNK):
        features, rows = [], []
        for i in range(start, start + PAIR_CHUNK):
            left = left_ref[pl.ds(i, 1), 0:64]
            left2 = jnp.concatenate([left, left], axis=1)
            scale = jnp.where(lane < 64, left2, -1.0)
            shift = jnp.where(lane < 64, 0.0, left2)
            features.append((right2_ref[...] * scale + shift).astype(BF16))
            rows.append(x_ref[i])
        mixed = dot32(
            jnp.concatenate([jnp.concatenate(rows, axis=0), jnp.concatenate(features, axis=0)], axis=1),
            mix_ref[...],
        )
        centred, updated = mixed[:, :128], mixed[:, 128:]
        variance = jnp.mean(centred * centred, axis=1, keepdims=True)
        normed = (centred * lax.rsqrt(variance + EPSILON)).astype(BF16)
        hidden = jnp.maximum(dot32(normed, wu_ref[...]), 0.0).astype(BF16)
        result = (updated + dot32(hidden, wd_ref[...])).astype(BF16)
        for i in range(PAIR_CHUNK):
            o_ref[start + i] = result[i * 256 : (i + 1) * 256]


def pair_transition(x, left, right, wp, wu, wd):
    rows = x.shape[0]

    def whole(array):
        return pl.BlockSpec(array.shape, lambda i: (0,) * array.ndim)

    return pl.pallas_call(
        pair_kernel,
        grid=(rows // PAIR_ROWS,),
        out_shape=jax.ShapeDtypeStruct(x.shape, BF16),
        in_specs=[
            pl.BlockSpec((PAIR_ROWS, 256, 128), lambda i: (i, 0, 0)),
            pl.BlockSpec((PAIR_ROWS, 128), lambda i: (i, 0)),
            whole(right),
            whole(wp),
            whole(wu),
            whole(wd),
        ],
        out_specs=pl.BlockSpec((PAIR_ROWS, 256, 128), lambda i: (i, 0, 0)),
        scratch_shapes=[pltpu.VMEM((256, 256), BF16), pltpu.VMEM((256, 128), F32)],
        compiler_params=pltpu.CompilerParams(dimension_semantics=("arbitrary",)),
    )(x, left, right, wp, wu, wd)


def body(seq_state, pair_state, w_bias, w_qkv, w_gate, w_out, w_seq_pair, w_pair_out, w_up, w_down):
    seq_out, left, right = front(seq_state, pair_state, w_bias, w_qkv, w_gate, w_out, w_seq_pair)
    return (seq_out, pair_transition(pair_state, left, right, w_pair_out, w_up, w_down))


def solution(mesh):
    return jax.shard_map(
        body,
        mesh=mesh,
        in_specs=(
            P("row", None),
            P("row", "col", None),
            P(),
            P(None, None, "col"),
            P(None, "col"),
            P(),
            P(),
            P(),
            P(),
            P(),
        ),
        out_specs=(P("row", None), P("row", "col", None)),
        check_vma=False,
    )
```

```python
import functools
import math

import jax
import jax.numpy as jnp
from jax import lax
from jax.experimental import pallas as pl
from jax.experimental.pallas import tpu as pltpu
from jax.sharding import PartitionSpec as P

EPSILON = 1e-05
F32 = jnp.float32
BF16 = jnp.bfloat16
PAIR_ROWS = 16
PAIR_CHUNK = 4
SCALE = 1.0 / math.sqrt(32)
NT = (((1,), (1,)), ((), ()))
NEAR_FIRST = (1, 7, 2, 6, 3, 5, 4)


def dot32(a, b):
    return jnp.dot(a, b, preferred_element_type=F32)


def dot_nt(a, b):
    return lax.dot_general(a, b, NT, preferred_element_type=F32)


def norm_rows(values):
    centred = values - jnp.mean(values, axis=-1, keepdims=True)
    variance = jnp.mean(centred * centred, axis=-1, keepdims=True)
    return centred * lax.rsqrt(variance + EPSILON)


def front_kernel(
    seq_hbm, pair_hbm, wbias_hbm, wqkv_hbm, wgate_hbm, wout_hbm, wsp_hbm,
    seq_out_ref, left_ref, right_ref,
    seq_v, pair_v, wbias_v, wqkv_v, wgate_v, wout_v, wsp_v,
    seq32, zbuf, qbuf, gsend, grecv, kv, bias_v, o32, osend, orecv, m_c, l_c, mlsend, mlrecv,
    lrsend, lbuf, rbuf, sosend, sobuf,
    in_sem, pair_sem,
    z_s, z_r, q_s, q_r, g_s, g_r, a_s, kv_r, d_s, o_s, o_r, ml_s, ml_r, l_s, l_r, r_s, r_r, so_s, so_r,
):
    row = lax.axis_index("row")
    col = lax.axis_index("col")
    core = lax.rem(row, 2)
    z = lax.rem(row // 2, 8)
    xh = row // 16
    partner = row + 1 - 2 * core
    own_plane = xh == col // 4
    own_right = row // 4 == col

    loads = [
        pltpu.make_async_copy(src, dst, in_sem.at[n])
        for n, (src, dst) in enumerate(
            ((seq_hbm, seq_v), (wqkv_hbm, wqkv_v), (wgate_hbm, wgate_v), (wbias_hbm, wbias_v),
             (wout_hbm, wout_v), (wsp_hbm, wsp_v))
        )
    ]
    for n in range(4):
        loads[n].start()

    barrier = pltpu.get_barrier_semaphore()

    def greet(r, c):
        pl.semaphore_signal(barrier, inc=1, device_id=(r, c), device_id_type=pl.DeviceIdType.MESH)

    def z_row(k):
        return xh * 16 + lax.rem(z + k, 8) * 2 + core

    for d in range(1, 8):
        greet(z_row(d), col)
        greet(row, lax.rem(col + d, 8))
    greet(partner, col)
    plane_row = (col // 4) * 16 + z * 2 + core
    for c in range(8):
        @pl.when(jnp.logical_not(jnp.logical_and(own_plane, col == c)))
        def _():
            greet(plane_row, c)

    @pl.loop(0, 32)
    def _(n):
        r, c = 4 * col + n // 8, lax.rem(n, 8)

        @pl.when(jnp.logical_not(jnp.logical_and(own_right, jnp.logical_and(row == r, col == c))))
        def _():
            greet(r, c)

    def pair_load(n):
        return pltpu.make_async_copy(pair_hbm.at[pl.ds(n * 8, 8)], pair_v.at[pl.ds(n * 8, 8)], pair_sem.at[n])

    for n in range(8):
        pair_load(n).start()
    for n in (4, 5):
        loads[n].start()

    lane = lax.broadcasted_iota(jnp.int32, (1, 128), 1)
    loads[0].wait()
    x = seq_v[...].astype(F32)
    seq32[...] = x
    normed = norm_rows(x).astype(BF16)
    loads[1].wait()
    zbuf[0, 0:64] = dot32(normed, wqkv_v[1]).astype(BF16)
    zbuf[0, 64:128] = dot32(normed, wqkv_v[2]).astype(BF16)
    qbuf[0] = dot32(normed, wqkv_v[0]).astype(BF16)

    pl.semaphore_wait(
        barrier, 15 + 8 - own_plane.astype(jnp.int32) + 32 - own_right.astype(jnp.int32)
    )

    def remote(src, dst, ss, rs, r, c):
        return pltpu.make_async_remote_copy(
            src_ref=src, dst_ref=dst, send_sem=ss, recv_sem=rs, device_id=(r, c),
            device_id_type=pl.DeviceIdType.MESH,
        )

    def z_copy(d):
        return remote(zbuf.at[0], zbuf.at[d], z_s.at[d], z_r.at[d], z_row(d), col)

    def col_copy(src, dst, ss, rs, d):
        return remote(src, dst, ss.at[d], rs.at[d], row, lax.rem(col + d, 8))

    def q_copy(d):
        return col_copy(qbuf.at[0], qbuf.at[d], q_s, q_r, d)

    def g_copy(d):
        return col_copy(gsend.at[lax.rem(col + d, 8)], grecv.at[d], g_s, g_r, d)

    for d in NEAR_FIRST:
        z_copy(d).start()

    loads[2].wait()
    gate = jax.nn.sigmoid(dot32(normed, wgate_v[...]))
    gsend[...] = gate.reshape(8, 8, 128)

    loads[3].wait()
    wb_t = wbias_v[...]
    ia = lax.broadcasted_iota(jnp.int32, (128, 128), 0)
    ib = lax.broadcasted_iota(jnp.int32, (128, 128), 1)
    centre = (jnp.where(ia == ib, 1.0, 0.0) - 1.0 / 128).astype(BF16)

    def bias_rows(n):
        pair_load(n).wait()
        c = dot32(pair_v[n * 8 : n * 8 + 8].reshape(2048, 128), centre)
        variance = jnp.mean(c * c, axis=1, keepdims=True)
        b = dot_nt(wb_t, (c * lax.rsqrt(variance + EPSILON)).astype(BF16)).astype(BF16).astype(F32)
        for i in range(8):
            for half in range(2):
                at = i * 256 + half * 128
                bias_v[half, pl.ds(n * 8 + i, 32, stride=64), :] = b[:, at : at + 128]

    def plane_copy(d, k):
        source = lax.rem(z + 8 - d, 8)
        return remote(
            zbuf.at[d], kv.at[lax.rem(source, 2) * 2 + core, col], a_s.at[d, k],
            kv_r.at[lax.rem(source, 2) * 2 + core, col], k * 16 + z * 2 + core, xh * 4 + source // 2,
        )

    def to_self(d, k):
        source = lax.rem(z + 8 - d, 8)
        return jnp.logical_and(xh == k, col == xh * 4 + source // 2)

    def forward(d):
        if d:
            z_copy(d).wait_recv()
        for k in range(2):
            here = to_self(d, k)

            @pl.when(here)
            def _():
                kv[lax.rem(z + 8 - d, 2) * 2 + core, col] = zbuf[d]

            @pl.when(jnp.logical_not(here))
            def _():
                plane_copy(d, k).start()

    forward(0)
    for e in NEAR_FIRST:
        q_copy(e).start()
    for e in NEAR_FIRST:
        g_copy(e).start()
    bias_rows(0)
    for n, pair in enumerate(((1, 7), (2, 6), (3, 5), (4,))):
        for d in pair:
            forward(d)
        bias_rows(n + 1)
    for n in range(5, 8):
        bias_rows(n)

    def kv_wait(q, c):
        return remote(kv.at[q, c], kv.at[q, c], d_s.at[0, 0], kv_r.at[q, c], partner, col)

    def core_copy(h, c):
        q = h * 2 + core
        return remote(kv.at[q, c], kv.at[q, c], d_s.at[h, c], kv_r.at[q, c], partner, col)

    for h in range(2):
        @pl.loop(0, 8)
        def _(c):
            @pl.when(jnp.logical_not(jnp.logical_and(own_plane, col == c)))
            def _():
                kv_wait(h * 2 + core, c).wait_recv()

            core_copy(h, c).start()

    for d in range(1, 8):
        q_copy(d).wait_recv()
    for h in range(2):
        @pl.loop(0, 8)
        def _(c):
            kv_wait(h * 2 + 1 - core, c).wait_recv()

    m_c[...] = jnp.zeros_like(m_c)
    l_c[...] = jnp.ones_like(l_c)
    head_of = lane // 32

    @pl.loop(0, 8, unroll=4)
    def _(d):
        g = lax.rem(col + 8 - d, 8)
        q = qbuf[d].astype(F32)
        q4 = jnp.concatenate([jnp.where(head_of == t, q, 0.0) for t in range(4)], axis=0).astype(BF16)
        blocks = [kv[b, g] for b in range(4)]
        keys = jnp.concatenate([b[0:64] for b in blocks], axis=0)
        values = jnp.concatenate([b[64:128] for b in blocks], axis=0)
        at = pl.ds(pl.multiple_of(g * 256, 256), 256)
        bias = jnp.concatenate([bias_v[0, at], bias_v[1, at]], axis=1)
        scores = dot_nt(q4, keys) * SCALE + bias
        peak = jnp.max(scores, axis=1, keepdims=True)
        weights = jnp.exp(scores - peak)
        total = jnp.sum(weights, axis=1, keepdims=True)
        o4 = dot32(weights.astype(BF16), values)
        out = jnp.zeros((64, 128), F32)
        m, l = m_c[...], l_c[...]
        for t in range(4):
            part = slice(t * 64, t * 64 + 64)
            out = jnp.where(head_of == t, o4[part], out)
            m = jnp.where(lane == g * 4 + t, peak[part], m)
            l = jnp.where(lane == g * 4 + t, total[part], l)
        m_c[...] = m
        l_c[...] = l
        o32[:, pl.ds(pl.multiple_of(g * 8, 8), 8), :] = out.reshape(8, 8, 128)

    osend[...] = o32[...].astype(BF16)
    mlsend[:, 0:8] = m_c[...].reshape(8, 8, 128)
    mlsend[:, 8:16] = l_c[...].reshape(8, 8, 128)

    def o_copy(d):
        return col_copy(osend.at[lax.rem(col + d, 8)], orecv.at[d], o_s, o_r, d)

    def ml_copy(d):
        return col_copy(mlsend.at[lax.rem(col + d, 8)], mlrecv.at[d], ml_s, ml_r, d)

    for d in (4, 3, 5, 2, 6, 1, 7):
        ml_copy(d).start()
        o_copy(d).start()
    orecv[0] = osend[col]
    mlrecv[0] = mlsend[col]
    grecv[0] = gsend[col]
    ea = lax.broadcasted_iota(jnp.int32, (128, 1024), 0)
    eb = lax.broadcasted_iota(jnp.int32, (128, 1024), 1)
    expand = jnp.where(ea == eb // 32, 1.0, 0.0).astype(BF16)
    for d in range(1, 8):
        g_copy(d).wait_recv()
        ml_copy(d).wait_recv()
        o_copy(d).wait_recv()

    peaks = [mlrecv[p, 0:8] for p in range(8)]
    top = functools.reduce(jnp.maximum, peaks)
    shares = [jnp.exp(v - top) for v in peaks]
    whole = functools.reduce(jnp.add, [s * mlrecv[p, 8:16] for p, s in enumerate(shares)])
    share = jnp.concatenate([s / whole for s in shares], axis=0)
    high = share.astype(BF16)
    low = (share - high.astype(F32)).astype(BF16)
    wide = dot32(high, expand) + dot32(low, expand)
    parts = []
    for g in range(8):
        tile = jnp.zeros((8, 128), F32)
        for p in range(8):
            tile = tile + wide[p * 8 : p * 8 + 8, g * 128 : g * 128 + 128] * orecv[p].astype(F32)[g * 8 : g * 8 + 8]
        parts.append(tile * grecv[lax.rem(col + 8 - g, 8)])
    attended = jnp.concatenate(parts, axis=1).astype(BF16)
    loads[4].wait()
    update = dot32(attended, wout_v[...])
    new_seq = (seq32[pl.ds(pl.multiple_of(col * 8, 8), 8), :] + update).astype(BF16).astype(F32)
    new_normed = norm_rows(new_seq).astype(BF16)
    loads[5].wait()
    sides = dot32(new_normed, wsp_v[...]).astype(BF16).astype(F32)
    lrsend[...] = sides

    def r_copy(n):
        return remote(lrsend, rbuf.at[lax.rem(row, 4), col], r_s.at[n], r_r.at[lax.rem(row, 4), col], n, row // 4)

    def l_copy(d):
        return remote(lrsend, lbuf.at[col], l_s.at[d], l_r.at[col], row, lax.rem(col + d, 8))

    def so_copy(d):
        return remote(sosend, sobuf.at[col], so_s.at[d], so_r.at[col], row, lax.rem(col + d, 8))

    def right_here(n):
        return jnp.logical_and(own_right, row == n)

    @pl.loop(0, 32)
    def _(n):
        @pl.when(jnp.logical_not(right_here(n)))
        def _():
            r_copy(n).start()

    for d in (4, 3, 5, 2, 6, 1, 7):
        l_copy(d).start()
    sosend[...] = jnp.concatenate([new_seq[:, g * 128 : g * 128 + 128] for g in range(8)], axis=0).astype(BF16)
    for d in (4, 3, 5, 2, 6, 1, 7):
        so_copy(d).start()
    lbuf[col] = sides
    sobuf[col] = sosend[...]

    @pl.when(own_right)
    def _():
        rbuf[lax.rem(row, 4), col] = sides

    for d in range(1, 8):
        z_copy(d).wait_send()
        q_copy(d).wait_send()
        g_copy(d).wait_send()
        ml_copy(d).wait_send()
        o_copy(d).wait_send()
    for d in range(8):
        for k in range(2):
            @pl.when(jnp.logical_not(to_self(d, k)))
            def _():
                plane_copy(d, k).wait_send()
    for h in range(2):
        @pl.loop(0, 8)
        def _(c):
            core_copy(h, c).wait_send()

    def col_wait(buf, ss, rs, d):
        source = lax.rem(col + 8 - d, 8)
        return remote(buf.at[source], buf.at[source], ss.at[d], rs.at[source], row, source)

    for d in range(1, 8):
        col_wait(lbuf, l_s, l_r, d).wait_recv()
        col_wait(sobuf, so_s, so_r, d).wait_recv()
    left_ref[...] = lbuf[...].reshape(64, 128)
    for c in range(8):
        block = sobuf[c].astype(F32)
        o32[c] = block
    seq_out_ref[...] = jnp.concatenate(
        [o32[:, g * 8 : g * 8 + 8, :].reshape(64, 128) for g in range(8)], axis=1
    ).astype(BF16)
    for q in range(4):
        @pl.loop(0, 8)
        def _(c):
            @pl.when(jnp.logical_not(jnp.logical_and(own_right, jnp.logical_and(lax.rem(row, 4) == q, col == c))))
            def _():
                remote(rbuf.at[q, c], rbuf.at[q, c], r_s.at[0], r_r.at[q, c], partner, col).wait_recv()

    right_ref[...] = rbuf[...].reshape(256, 128)
    for d in range(1, 8):
        l_copy(d).wait_send()
        so_copy(d).wait_send()

    @pl.loop(0, 32)
    def _(n):
        @pl.when(jnp.logical_not(right_here(n)))
        def _():
            r_copy(n).wait_send()


def front(seq_state, pair_state, w_bias, w_qkv, w_gate, w_out, w_seq_pair):
    any_spec = pl.BlockSpec(memory_space=pl.ANY)
    vmem_spec = pl.BlockSpec(memory_space=pltpu.VMEM)
    dma = pltpu.SemaphoreType.DMA
    return pl.pallas_call(
        front_kernel,
        out_shape=(
            jax.ShapeDtypeStruct((64, 1024), BF16),
            jax.ShapeDtypeStruct((64, 128), F32),
            jax.ShapeDtypeStruct((256, 128), F32),
        ),
        in_specs=[any_spec] * 7,
        out_specs=(vmem_spec,) * 3,
        scratch_shapes=[
            pltpu.VMEM((64, 1024), BF16),
            pltpu.VMEM((64, 256, 128), BF16),
            pltpu.VMEM((32, 128), BF16),
            pltpu.VMEM((3, 1024, 128), BF16),
            pltpu.VMEM((1024, 128), BF16),
            pltpu.VMEM((1024, 1024), BF16),
            pltpu.VMEM((1024, 128), BF16),
            pltpu.VMEM((64, 1024), F32),
            pltpu.VMEM((8, 128, 128), BF16),
            pltpu.VMEM((8, 64, 128), BF16),
            pltpu.VMEM((8, 8, 128), F32),
            pltpu.VMEM((8, 8, 128), F32),
            pltpu.VMEM((4, 8, 128, 128), BF16),
            pltpu.VMEM((2, 2048, 128), F32),
            pltpu.VMEM((8, 64, 128), F32),
            pltpu.VMEM((8, 64, 128), BF16),
            pltpu.VMEM((8, 64, 128), BF16),
            pltpu.VMEM((64, 128), F32),
            pltpu.VMEM((64, 128), F32),
            pltpu.VMEM((8, 16, 128), F32),
            pltpu.VMEM((8, 16, 128), F32),
            pltpu.VMEM((8, 128), F32),
            pltpu.VMEM((8, 8, 128), F32),
            pltpu.VMEM((4, 8, 8, 128), F32),
            pltpu.VMEM((64, 128), BF16),
            pltpu.VMEM((8, 64, 128), BF16),
            dma((6,)), dma((8,)),
            dma((8,)), dma((8,)), dma((8,)), dma((8,)), dma((8,)), dma((8,)),
            dma((8, 2)), dma((4, 8)), dma((2, 8)),
            dma((8,)), dma((8,)), dma((8,)), dma((8,)), dma((8,)), dma((8,)),
            dma((32,)), dma((4, 8)), dma((8,)), dma((8,)),
        ],
        compiler_params=pltpu.CompilerParams(
            collective_id=0, has_side_effects=True, vmem_limit_bytes=67_043_328
        ),
        cost_estimate=pl.CostEstimate(flops=3_000_000_000, bytes_accessed=8_000_000, transcendentals=600_000),
    )(seq_state, pair_state, w_bias, w_qkv, w_gate, w_out, w_seq_pair)


def pair_kernel(x_ref, left_ref, right_ref, wp_ref, wu_ref, wd_ref, o_ref, mix_ref, right2_ref):
    @pl.when(pl.program_id(0) == 0)
    def _():
        w = wp_ref[...].astype(F32)
        centred = w - jnp.mean(w, axis=1, keepdims=True)
        a = lax.broadcasted_iota(jnp.int32, (128, 128), 0)
        b = lax.broadcasted_iota(jnp.int32, (128, 128), 1)
        eye = jnp.where(a == b, 1.0, 0.0)
        mix_ref[0:128, 0:128] = (eye - 1.0 / 128).astype(BF16)
        mix_ref[0:128, 128:256] = eye.astype(BF16)
        mix_ref[128:256, 0:128] = centred.astype(BF16)
        mix_ref[128:256, 128:256] = wp_ref[...]
        r = right_ref[:, 64:128]
        right2_ref[...] = jnp.concatenate([r, r], axis=1)

    lane = lax.broadcasted_iota(jnp.int32, (1, 128), 1)
    for start in range(0, PAIR_ROWS, PAIR_CHUNK):
        features, rows = [], []
        for i in range(start, start + PAIR_CHUNK):
            left = left_ref[pl.ds(i, 1), 0:64]
            left2 = jnp.concatenate([left, left], axis=1)
            scale = jnp.where(lane < 64, left2, -1.0)
            shift = jnp.where(lane < 64, 0.0, left2)
            features.append((right2_ref[...] * scale + shift).astype(BF16))
            rows.append(x_ref[i])
        mixed = dot32(
            jnp.concatenate([jnp.concatenate(rows, axis=0), jnp.concatenate(features, axis=0)], axis=1),
            mix_ref[...],
        )
        centred, updated = mixed[:, :128], mixed[:, 128:]
        variance = jnp.mean(centred * centred, axis=1, keepdims=True)
        normed = (centred * lax.rsqrt(variance + EPSILON)).astype(BF16)
        hidden = jnp.maximum(dot32(normed, wu_ref[...]), 0.0).astype(BF16)
        result = (updated + dot32(hidden, wd_ref[...])).astype(BF16)
        for i in range(PAIR_CHUNK):
            o_ref[start + i] = result[i * 256 : (i + 1) * 256]


def pair_transition(x, left, right, wp, wu, wd):
    rows = x.shape[0]

    def whole(array):
        return pl.BlockSpec(array.shape, lambda i: (0,) * array.ndim)

    return pl.pallas_call(
        pair_kernel,
        grid=(rows // PAIR_ROWS,),
        out_shape=jax.ShapeDtypeStruct(x.shape, BF16),
        in_specs=[
            pl.BlockSpec((PAIR_ROWS, 256, 128), lambda i: (i, 0, 0)),
            pl.BlockSpec((PAIR_ROWS, 128), lambda i: (i, 0)),
            whole(right),
            whole(wp),
            whole(wu),
            whole(wd),
        ],
        out_specs=pl.BlockSpec((PAIR_ROWS, 256, 128), lambda i: (i, 0, 0)),
        scratch_shapes=[pltpu.VMEM((256, 256), BF16), pltpu.VMEM((256, 128), F32)],
        compiler_params=pltpu.CompilerParams(dimension_semantics=("arbitrary",)),
    )(x, left, right, wp, wu, wd)


def body(seq_state, pair_state, w_bias, w_qkv, w_gate, w_out, w_seq_pair, w_pair_out, w_up, w_down):
    seq_out, left, right = front(seq_state, pair_state, w_bias.T, w_qkv, w_gate, w_out, w_seq_pair)
    return (seq_out, pair_transition(pair_state, left, right, w_pair_out, w_up, w_down))


def solution(mesh):
    return jax.shard_map(
        body,
        mesh=mesh,
        in_specs=(
            P("row", None),
            P("row", "col", None),
            P(),
            P(None, None, "col"),
            P(None, "col"),
            P(),
            P(),
            P(),
            P(),
            P(),
        ),
        out_specs=(P("row", None), P("row", "col", None)),
        check_vma=False,
    )
```

```python
import functools
import math

import jax
import jax.numpy as jnp
from jax import lax
from jax.experimental import pallas as pl
from jax.experimental.pallas import tpu as pltpu
from jax.sharding import PartitionSpec as P

EPSILON = 1e-05
F32 = jnp.float32
BF16 = jnp.bfloat16
PAIR_ROWS = 16
PAIR_CHUNK = 4
SCALE = 1.0 / math.sqrt(32)
NT = (((1,), (1,)), ((), ()))
NEAR_FIRST = (1, 7, 2, 6, 3, 5, 4)
FAR_FIRST = (3, 5, 4, 2, 1, 7, 6)


def dot32(a, b):
    return jnp.dot(a, b, preferred_element_type=F32)


def dot_nt(a, b):
    return lax.dot_general(a, b, NT, preferred_element_type=F32)


def norm_rows(values):
    centred = values - jnp.mean(values, axis=-1, keepdims=True)
    variance = jnp.mean(centred * centred, axis=-1, keepdims=True)
    return centred * lax.rsqrt(variance + EPSILON)


def front_kernel(
    seq_hbm, pair_hbm, wbias_hbm, wqkv_hbm, wgate_hbm, wout_hbm, wsp_hbm,
    sobuf, lbuf, rbuf,
    seq_v, pair_v, wbias_v, wqkv_v, wgate_v, wout_v, wsp_v,
    seq32, zbuf, qbuf, gsend, grecv, kv, bias_v, o32, osend, orecv, ml_c, mlsend, mlrecv,
    lrsend, sosend,
    in_sem, pair_sem, own_sem,
    z_s, z_r, q_s, q_r, g_s, g_r, a_s, kv_r, d_s, o_s, o_r, ml_s, ml_r, l_s, l_r, r_s, r_r, so_s, so_r,
):
    row = lax.axis_index("row")
    col = lax.axis_index("col")
    core = lax.rem(row, 2)
    z = lax.rem(row // 2, 8)
    xh = row // 16
    partner = row + 1 - 2 * core
    own_plane = xh == col // 4
    own_right = row // 4 == col

    loads = [
        pltpu.make_async_copy(src, dst, in_sem.at[n])
        for n, (src, dst) in enumerate(
            ((seq_hbm, seq_v), (wqkv_hbm, wqkv_v), (wgate_hbm, wgate_v), (wbias_hbm, wbias_v),
             (wout_hbm, wout_v), (wsp_hbm, wsp_v))
        )
    ]
    for n in range(4):
        loads[n].start()

    barrier = pltpu.get_barrier_semaphore()

    def greet(r, c):
        pl.semaphore_signal(barrier, inc=1, device_id=(r, c), device_id_type=pl.DeviceIdType.MESH)

    def z_row(k):
        return xh * 16 + lax.rem(z + k, 8) * 2 + core

    for d in range(1, 8):
        greet(z_row(d), col)
        greet(row, lax.rem(col + d, 8))
    greet(partner, col)
    plane_row = (col // 4) * 16 + z * 2 + core
    for c in range(8):
        @pl.when(jnp.logical_not(jnp.logical_and(own_plane, col == c)))
        def _():
            greet(plane_row, c)

    @pl.loop(0, 32)
    def _(n):
        r, c = 4 * col + n // 8, lax.rem(n, 8)

        @pl.when(jnp.logical_not(jnp.logical_and(own_right, jnp.logical_and(row == r, col == c))))
        def _():
            greet(r, c)

    def pair_load(n):
        return pltpu.make_async_copy(pair_hbm.at[pl.ds(n * 8, 8)], pair_v.at[pl.ds(n * 8, 8)], pair_sem.at[n])

    for n in range(8):
        pair_load(n).start()
    for n in (4, 5):
        loads[n].start()

    lane = lax.broadcasted_iota(jnp.int32, (1, 128), 1)
    loads[0].wait()
    x = seq_v[...].astype(F32)
    seq32[...] = x
    normed = norm_rows(x).astype(BF16)
    loads[1].wait()
    zbuf[0, 0:64] = dot32(normed, wqkv_v[1]).astype(BF16)
    zbuf[0, 64:128] = dot32(normed, wqkv_v[2]).astype(BF16)

    pl.semaphore_wait(
        barrier, 15 + 8 - own_plane.astype(jnp.int32) + 32 - own_right.astype(jnp.int32)
    )

    def remote(src, dst, ss, rs, r, c):
        return pltpu.make_async_remote_copy(
            src_ref=src, dst_ref=dst, send_sem=ss, recv_sem=rs, device_id=(r, c),
            device_id_type=pl.DeviceIdType.MESH,
        )

    def z_copy(d):
        return remote(zbuf.at[0], zbuf.at[d], z_s.at[d], z_r.at[d], z_row(d), col)

    def col_copy(src, dst, ss, rs, d):
        return remote(src, dst, ss.at[d], rs.at[d], row, lax.rem(col + d, 8))

    def q_copy(d):
        return col_copy(qbuf.at[0], qbuf.at[d], q_s, q_r, d)

    def g_copy(d):
        return col_copy(gsend.at[lax.rem(col + d, 8)], grecv.at[d], g_s, g_r, d)

    turned = lax.rem(col, 2) == 1
    late = lax.rem(col // 2, 2) == 1

    def turn(k):
        d = jnp.where(late, FAR_FIRST[k], NEAR_FIRST[k])
        return jnp.where(turned, 8 - d, d)

    for k in range(7):
        z_copy(turn(k)).start()
    qbuf[0] = dot32(normed, wqkv_v[0]).astype(BF16)

    loads[2].wait()
    gate = jax.nn.sigmoid(dot32(normed, wgate_v[...]))
    gsend[...] = gate.reshape(8, 8, 128)

    loads[3].wait()
    wb_t = wbias_v[...]
    ia = lax.broadcasted_iota(jnp.int32, (128, 128), 0)
    ib = lax.broadcasted_iota(jnp.int32, (128, 128), 1)
    centre = (jnp.where(ia == ib, 1.0, 0.0) - 1.0 / 128).astype(BF16)

    def bias_rows(n):
        pair_load(n).wait()
        c = dot32(pair_v[n * 8 : n * 8 + 8].reshape(2048, 128), centre)
        variance = jnp.mean(c * c, axis=1, keepdims=True)
        b = dot_nt(wb_t, (c * lax.rsqrt(variance + EPSILON)).astype(BF16)).astype(BF16).astype(F32)
        for i in range(8):
            for half in range(2):
                at = i * 256 + half * 128
                bias_v[half, pl.ds(n * 8 + i, 32, stride=64), :] = b[:, at : at + 128]

    def plane_copy(d, k):
        source = lax.rem(z + 8 - d, 8)
        return remote(
            zbuf.at[d], kv.at[lax.rem(source, 2) * 2 + core, col], a_s.at[d, k],
            kv_r.at[lax.rem(source, 2) * 2 + core, col], k * 16 + z * 2 + core, xh * 4 + source // 2,
        )

    def to_self(d, k):
        source = lax.rem(z + 8 - d, 8)
        return jnp.logical_and(xh == k, col == xh * 4 + source // 2)

    def forward(d):
        for k in range(2):
            here = to_self(d, k)

            @pl.when(here)
            def _():
                kv[lax.rem(z + 8 - d, 2) * 2 + core, col] = zbuf[d]

            @pl.when(jnp.logical_not(here))
            def _():
                plane_copy(d, k).start()

    forward(0)
    for e in NEAR_FIRST:
        q_copy(e).start()
    for e in NEAR_FIRST:
        g_copy(e).start()
    bias_rows(0)
    for k in range(7):
        z_copy(turn(k)).wait_recv()
        forward(turn(k))
        if k % 2:
            bias_rows(k // 2 + 1)
    bias_rows(4)
    for n in range(5, 8):
        bias_rows(n)

    def kv_wait(q, c):
        return remote(kv.at[q, c], kv.at[q, c], d_s.at[0, 0], kv_r.at[q, c], partner, col)

    def core_copy(h, c):
        q = h * 2 + core
        return remote(kv.at[q, c], kv.at[q, c], d_s.at[h, c], kv_r.at[q, c], partner, col)

    @pl.loop(0, 8)
    def _(d):
        c = lax.rem(col + 8 - d, 8)
        for h in range(2):
            @pl.when(jnp.logical_not(jnp.logical_and(own_plane, col == c)))
            def _():
                kv_wait(h * 2 + core, c).wait_recv()

            core_copy(h, c).start()

    for d in range(1, 8):
        q_copy(d).wait_recv()

    ml_c[...] = jnp.zeros_like(ml_c)
    head_of = lane // 32

    @pl.loop(0, 8, unroll=4)
    def _(d):
        g = lax.rem(col + 8 - d, 8)
        for h in range(2):
            kv_wait(h * 2 + 1 - core, g).wait_recv()
        q = qbuf[d].astype(F32)
        q4 = jnp.concatenate([jnp.where(head_of == t, q, 0.0) for t in range(4)], axis=0).astype(BF16)
        blocks = [kv[b, g] for b in range(4)]
        keys = jnp.concatenate([b[0:64] for b in blocks], axis=0)
        values = jnp.concatenate([b[64:128] for b in blocks], axis=0)
        at = pl.ds(pl.multiple_of(g * 256, 256), 256)
        bias = jnp.concatenate([bias_v[0, at], bias_v[1, at]], axis=1)
        scores = dot_nt(q4, keys) * SCALE + bias
        peak = jnp.max(scores, axis=1, keepdims=True)
        weights = jnp.exp(scores - peak)
        total = jnp.sum(weights, axis=1, keepdims=True)
        o4 = dot32(weights.astype(BF16), values)
        out = jnp.zeros((64, 128), F32)
        ml = ml_c[...]
        for t in range(4):
            part = slice(t * 64, t * 64 + 64)
            out = jnp.where(head_of == t, o4[part], out)
            ml = jnp.where(lane == g * 4 + t, peak[part], jnp.where(lane == 32 + g * 4 + t, total[part], ml))
        ml_c[...] = ml
        o32[:, pl.ds(pl.multiple_of(g * 8, 8), 8), :] = out.reshape(8, 8, 128)

    osend[...] = o32[...].astype(BF16)
    mlsend[...] = ml_c[...].reshape(8, 8, 128)

    def o_copy(d):
        return col_copy(osend.at[lax.rem(col + d, 8)], orecv.at[d], o_s, o_r, d)

    def ml_copy(d):
        return col_copy(mlsend.at[lax.rem(col + d, 8)], mlrecv.at[d], ml_s, ml_r, d)

    for d in (4, 3, 5, 2, 6, 1, 7):
        ml_copy(d).start()
        o_copy(d).start()
    orecv[0] = osend[col]
    mlrecv[0] = mlsend[col]
    grecv[0] = gsend[col]
    ea = lax.broadcasted_iota(jnp.int32, (128, 1024), 0)
    eb = lax.broadcasted_iota(jnp.int32, (128, 1024), 1)
    expand = jnp.where(ea == eb // 32, 1.0, 0.0).astype(BF16)
    for d in range(1, 8):
        g_copy(d).wait_recv()
        ml_copy(d).wait_recv()
        o_copy(d).wait_recv()

    peaks = [mlrecv[p] for p in range(8)]
    sums = [pltpu.roll(v, 96, 1) for v in peaks]
    partials = [orecv[p].astype(F32) for p in range(8)]
    top = functools.reduce(jnp.maximum, peaks)
    shares = [jnp.exp(v - top) for v in peaks]
    whole = functools.reduce(jnp.add, [s * v for s, v in zip(shares, sums)])
    share = jnp.concatenate([jnp.where(lane < 32, s / whole, 0.0) for s in shares], axis=0)
    high = share.astype(BF16)
    low = (share - high.astype(F32)).astype(BF16)
    wide = dot32(high, expand) + dot32(low, expand)
    parts = []
    for g in range(8):
        tile = jnp.zeros((8, 128), F32)
        for p in range(8):
            tile = tile + wide[p * 8 : p * 8 + 8, g * 128 : g * 128 + 128] * partials[p][g * 8 : g * 8 + 8]
        parts.append(tile * grecv[lax.rem(col + 8 - g, 8)])
    attended = jnp.concatenate(parts, axis=1).astype(BF16)
    loads[4].wait()
    update = dot32(attended, wout_v[...])
    new_seq = (seq32[pl.ds(pl.multiple_of(col * 8, 8), 8), :] + update).astype(BF16).astype(F32)
    new_normed = norm_rows(new_seq).astype(BF16)
    loads[5].wait()
    sides = dot32(new_normed, wsp_v[...]).astype(BF16)
    lrsend[...] = sides

    def r_copy(n):
        return remote(lrsend, rbuf.at[lax.rem(row, 4), col], r_s.at[n], r_r.at[lax.rem(row, 4), col], n, row // 4)

    def l_copy(d):
        return remote(lrsend, lbuf.at[col], l_s.at[d], l_r.at[col], row, lax.rem(col + d, 8))

    def so_copy(d):
        return remote(sosend, sobuf.at[col], so_s.at[d], so_r.at[col], row, lax.rem(col + d, 8))

    def right_here(n):
        return jnp.logical_and(own_right, row == n)

    @pl.loop(0, 32)
    def _(j):
        far = j // 4
        far = 4 + (far + 1) // 2 * (1 - 2 * lax.rem(far, 2))
        n = lax.rem(j // 2, 2) * 16 + lax.rem(z + far, 8) * 2 + lax.rem(j, 2)

        @pl.when(jnp.logical_not(right_here(n)))
        def _():
            r_copy(n).start()

    for d in (4, 3, 5, 2, 6, 1, 7):
        l_copy(d).start()
    sosend[...] = jnp.concatenate([new_seq[:, g * 128 : g * 128 + 128] for g in range(8)], axis=0).astype(BF16)
    for d in (4, 3, 5, 2, 6, 1, 7):
        so_copy(d).start()
    own = [
        pltpu.make_async_copy(src, dst, own_sem.at[n])
        for n, (src, dst) in enumerate(
            ((lrsend, lbuf.at[col]), (sosend, sobuf.at[col]), (lrsend, rbuf.at[lax.rem(row, 4), col]))
        )
    ]
    own[0].start()
    own[1].start()

    @pl.when(own_right)
    def _():
        own[2].start()

    for d in range(1, 8):
        z_copy(d).wait_send()
        q_copy(d).wait_send()
        g_copy(d).wait_send()
        ml_copy(d).wait_send()
        o_copy(d).wait_send()
    for d in range(8):
        for k in range(2):
            @pl.when(jnp.logical_not(to_self(d, k)))
            def _():
                plane_copy(d, k).wait_send()
    for h in range(2):
        @pl.loop(0, 8)
        def _(c):
            core_copy(h, c).wait_send()

    for d in range(1, 8):
        l_copy(d).wait_send()
        so_copy(d).wait_send()

    @pl.loop(0, 32)
    def _(n):
        @pl.when(jnp.logical_not(right_here(n)))
        def _():
            r_copy(n).wait_send()

    own[0].wait()
    own[1].wait()

    @pl.when(own_right)
    def _():
        own[2].wait()

    def col_wait(buf, ss, rs, d):
        source = lax.rem(col + 8 - d, 8)
        return remote(buf.at[source], buf.at[source], ss.at[d], rs.at[source], row, source)

    for d in range(1, 8):
        col_wait(lbuf, l_s, l_r, d).wait_recv()
        col_wait(sobuf, so_s, so_r, d).wait_recv()

    @pl.loop(0, 32)
    def _(n):
        q, c = n // 8, lax.rem(n, 8)

        @pl.when(jnp.logical_not(jnp.logical_and(own_right, jnp.logical_and(lax.rem(row, 4) == q, col == c))))
        def _():
            remote(rbuf.at[q, c], rbuf.at[q, c], r_s.at[0], r_r.at[q, c], partner, col).wait_recv()


def front(seq_state, pair_state, w_bias, w_qkv, w_gate, w_out, w_seq_pair):
    any_spec = pl.BlockSpec(memory_space=pl.ANY)
    dma = pltpu.SemaphoreType.DMA
    return pl.pallas_call(
        front_kernel,
        out_shape=(
            jax.ShapeDtypeStruct((8, 64, 128), BF16),
            jax.ShapeDtypeStruct((8, 8, 128), BF16),
            jax.ShapeDtypeStruct((4, 8, 8, 128), BF16),
        ),
        in_specs=[any_spec] * 7,
        out_specs=(any_spec,) * 3,
        scratch_shapes=[
            pltpu.VMEM((64, 1024), BF16),
            pltpu.VMEM((64, 256, 128), BF16),
            pltpu.VMEM((32, 128), BF16),
            pltpu.VMEM((3, 1024, 128), BF16),
            pltpu.VMEM((1024, 128), BF16),
            pltpu.VMEM((1024, 1024), BF16),
            pltpu.VMEM((1024, 128), BF16),
            pltpu.VMEM((64, 1024), F32),
            pltpu.VMEM((8, 128, 128), BF16),
            pltpu.VMEM((8, 64, 128), BF16),
            pltpu.VMEM((8, 8, 128), F32),
            pltpu.VMEM((8, 8, 128), F32),
            pltpu.VMEM((4, 8, 128, 128), BF16),
            pltpu.VMEM((2, 2048, 128), F32),
            pltpu.VMEM((8, 64, 128), F32),
            pltpu.VMEM((8, 64, 128), BF16),
            pltpu.VMEM((8, 64, 128), BF16),
            pltpu.VMEM((64, 128), F32),
            pltpu.VMEM((8, 8, 128), F32),
            pltpu.VMEM((8, 8, 128), F32),
            pltpu.VMEM((8, 128), BF16),
            pltpu.VMEM((64, 128), BF16),
            dma((6,)), dma((8,)), dma((3,)),
            dma((8,)), dma((8,)), dma((8,)), dma((8,)), dma((8,)), dma((8,)),
            dma((8, 2)), dma((4, 8)), dma((2, 8)),
            dma((8,)), dma((8,)), dma((8,)), dma((8,)), dma((8,)), dma((8,)),
            dma((32,)), dma((4, 8)), dma((8,)), dma((8,)),
        ],
        compiler_params=pltpu.CompilerParams(
            collective_id=0, has_side_effects=True, vmem_limit_bytes=67_043_328
        ),
        cost_estimate=pl.CostEstimate(flops=3_000_000_000, bytes_accessed=8_000_000, transcendentals=600_000),
    )(seq_state, pair_state, w_bias, w_qkv, w_gate, w_out, w_seq_pair)


def pair_kernel(x_ref, left_ref, right_ref, wp_ref, wu_ref, wd_ref, seq_ref, o_ref, seq_out_ref, mix_ref, right2_ref):
    @pl.when(pl.program_id(0) == 0)
    def _():
        w = wp_ref[...].astype(F32)
        centred = w - jnp.mean(w, axis=1, keepdims=True)
        a = lax.broadcasted_iota(jnp.int32, (128, 128), 0)
        b = lax.broadcasted_iota(jnp.int32, (128, 128), 1)
        eye = jnp.where(a == b, 1.0, 0.0)
        mix_ref[0:128, 0:128] = (eye - 1.0 / 128).astype(BF16)
        mix_ref[0:128, 128:256] = eye.astype(BF16)
        mix_ref[128:256, 0:128] = centred.astype(BF16)
        mix_ref[128:256, 128:256] = wp_ref[...]
        r = right_ref[...].astype(F32).reshape(256, 128)[:, 64:128]
        right2_ref[...] = jnp.concatenate([r, r], axis=1).astype(BF16)
        rows = seq_ref[...].astype(F32)
        seq_out_ref[...] = jnp.concatenate(
            [rows[:, g * 8 : g * 8 + 8, :].reshape(64, 128) for g in range(8)], axis=1
        ).astype(BF16)

    lane = lax.broadcasted_iota(jnp.int32, (1, 128), 1)

    lefts = left_ref[...].astype(F32).reshape(PAIR_ROWS, 128)

    def update(start):
        features, rows = [], []
        for i in range(start, start + PAIR_CHUNK):
            left = lefts[i : i + 1, 0:64]
            left2 = jnp.concatenate([left, left], axis=1)
            scale = jnp.where(lane < 64, left2, -1.0).astype(BF16)
            shift = jnp.where(lane < 64, 0.0, left2).astype(BF16)
            features.append(right2_ref[...] * scale + shift)
            rows.append(x_ref[i])
        mixed = dot32(
            jnp.concatenate([jnp.concatenate(rows, axis=0), jnp.concatenate(features, axis=0)], axis=1),
            mix_ref[...],
        )
        return mixed[:, :128], mixed[:, 128:]

    def normed(centred):
        variance = jnp.mean(centred * centred, axis=1, keepdims=True)
        return (centred * lax.rsqrt(variance + EPSILON)).astype(BF16)

    def finish(start, hidden, updated):
        result = (updated + dot32(hidden, wd_ref[...])).astype(BF16)
        for i in range(PAIR_CHUNK):
            o_ref[start + i] = result[i * 256 : (i + 1) * 256]

    count = PAIR_ROWS // PAIR_CHUNK
    ready, updates, hidden = {}, {}, {}
    for t in range(count + 2):
        if t < count:
            centred, updates[t] = update(t * PAIR_CHUNK)
        if 0 <= t - 1 < count:
            hidden[t - 1] = jnp.maximum(dot32(ready[t - 1], wu_ref[...]).astype(BF16), 0)
        if t < count:
            ready[t] = normed(centred)
        if 0 <= t - 2:
            finish((t - 2) * PAIR_CHUNK, hidden[t - 2], updates[t - 2])


def pair_transition(x, left, right, wp, wu, wd, seq):
    rows = x.shape[0]

    def whole(shape):
        return pl.BlockSpec(shape, lambda i: (0,) * len(shape))

    return pl.pallas_call(
        pair_kernel,
        grid=(rows // PAIR_ROWS,),
        out_shape=(jax.ShapeDtypeStruct(x.shape, BF16), jax.ShapeDtypeStruct((64, 1024), BF16)),
        in_specs=[
            pl.BlockSpec((PAIR_ROWS, 256, 128), lambda i: (i, 0, 0)),
            pl.BlockSpec((PAIR_ROWS // 8, 8, 128), lambda i: (i, 0, 0)),
            whole(right.shape),
            whole(wp.shape),
            whole(wu.shape),
            whole(wd.shape),
            whole(seq.shape),
        ],
        out_specs=(pl.BlockSpec((PAIR_ROWS, 256, 128), lambda i: (i, 0, 0)), whole((64, 1024))),
        scratch_shapes=[pltpu.VMEM((256, 256), BF16), pltpu.VMEM((256, 128), BF16)],
        compiler_params=pltpu.CompilerParams(dimension_semantics=("arbitrary",)),
    )(x, left, right, wp, wu, wd, seq)


def body(seq_state, pair_state, w_bias, w_qkv, w_gate, w_out, w_seq_pair, w_pair_out, w_up, w_down):
    seq_rows, left, right = front(seq_state, pair_state, w_bias.T, w_qkv, w_gate, w_out, w_seq_pair)
    pair_out, seq_out = pair_transition(pair_state, left, right, w_pair_out, w_up, w_down, seq_rows)
    return (seq_out, pair_out)


def solution(mesh):
    return jax.shard_map(
        body,
        mesh=mesh,
        in_specs=(
            P("row", None),
            P("row", "col", None),
            P(),
            P(None, None, "col"),
            P(None, "col"),
            P(),
            P(),
            P(),
            P(),
            P(),
        ),
        out_specs=(P("row", None), P("row", "col", None)),
        check_vma=False,
    )
```

```python
import functools
import math

import jax
import jax.numpy as jnp
from jax import lax
from jax.experimental import pallas as pl
from jax.experimental.pallas import tpu as pltpu
from jax.sharding import PartitionSpec as P

EPSILON = 1e-05
F32 = jnp.float32
BF16 = jnp.bfloat16
PAIR_ROWS = 16
PAIR_CHUNK = 4
SCALE = 1.0 / math.sqrt(32)
NT = (((1,), (1,)), ((), ()))
NEAR_FIRST = (1, 7, 2, 6, 3, 5, 4)
FAR_FIRST = (3, 5, 4, 2, 1, 7, 6)


def dot32(a, b):
    return jnp.dot(a, b, preferred_element_type=F32)


def dot_nt(a, b):
    return lax.dot_general(a, b, NT, preferred_element_type=F32)


def norm_rows(values):
    centred = values - jnp.mean(values, axis=-1, keepdims=True)
    variance = jnp.mean(centred * centred, axis=-1, keepdims=True)
    return centred * lax.rsqrt(variance + EPSILON)


def front_kernel(
    seq_hbm, pair_hbm, wbias_hbm, wqkv_hbm, wgate_hbm, wout_hbm, wsp_hbm,
    sobuf, lbuf, rbuf,
    seq_v, pair_v, wbias_v, wqkv_v, wgate_v, wout_v, wsp_v,
    seq32, zbuf, qbuf, gsend, grecv, kv, bias_v, o32, osend, orecv, ml_c, mlsend, mlrecv,
    lrsend, sosend,
    in_sem, pair_sem, own_sem,
    z_s, z_r, q_s, q_r, g_s, g_r, a_s, kv_r, d_s, o_s, o_r, ml_s, ml_r, l_s, l_r, r_s, r_r, so_s, so_r,
):
    row = lax.axis_index("row")
    col = lax.axis_index("col")
    core = lax.rem(row, 2)
    z = lax.rem(row // 2, 8)
    xh = row // 16
    partner = row + 1 - 2 * core
    own_plane = xh == col // 4
    own_right = row // 4 == col

    loads = [
        pltpu.make_async_copy(src, dst, in_sem.at[n])
        for n, (src, dst) in enumerate(
            ((seq_hbm, seq_v), (wqkv_hbm, wqkv_v), (wgate_hbm, wgate_v), (wbias_hbm, wbias_v),
             (wout_hbm, wout_v), (wsp_hbm, wsp_v))
        )
    ]
    for n in range(4):
        loads[n].start()

    barrier = pltpu.get_barrier_semaphore()

    def greet(r, c):
        pl.semaphore_signal(barrier, inc=1, device_id=(r, c), device_id_type=pl.DeviceIdType.MESH)

    def z_row(k):
        return xh * 16 + lax.rem(z + k, 8) * 2 + core

    for d in range(1, 8):
        greet(z_row(d), col)
        greet(row, lax.rem(col + d, 8))
    greet(partner, col)
    plane_row = (col // 4) * 16 + z * 2 + core
    for c in range(8):
        @pl.when(jnp.logical_not(jnp.logical_and(own_plane, col == c)))
        def _():
            greet(plane_row, c)

    def pair_load(n):
        return pltpu.make_async_copy(pair_hbm.at[pl.ds(n * 8, 8)], pair_v.at[pl.ds(n * 8, 8)], pair_sem.at[n])

    lane = lax.broadcasted_iota(jnp.int32, (1, 128), 1)
    loads[0].wait()
    x = seq_v[...].astype(F32)
    seq32[...] = x
    normed = norm_rows(x).astype(BF16)
    loads[1].wait()
    for n in range(8):
        pair_load(n).start()
    for n in (4, 5):
        loads[n].start()
    zbuf[0, 0:64] = dot32(normed, wqkv_v[1]).astype(BF16)
    zbuf[0, 64:128] = dot32(normed, wqkv_v[2]).astype(BF16)

    pl.semaphore_wait(barrier, 15 + 8 - own_plane.astype(jnp.int32))

    def remote(src, dst, ss, rs, r, c):
        return pltpu.make_async_remote_copy(
            src_ref=src, dst_ref=dst, send_sem=ss, recv_sem=rs, device_id=(r, c),
            device_id_type=pl.DeviceIdType.MESH,
        )

    def z_copy(d):
        return remote(zbuf.at[0], zbuf.at[d], z_s.at[d], z_r.at[d], z_row(d), col)

    def col_copy(src, dst, ss, rs, d):
        return remote(src, dst, ss.at[d], rs.at[d], row, lax.rem(col + d, 8))

    def q_copy(d):
        return col_copy(qbuf.at[0], qbuf.at[d], q_s, q_r, d)

    def g_copy(d):
        return col_copy(gsend.at[lax.rem(col + d, 8)], grecv.at[d], g_s, g_r, d)

    turned = lax.rem(col, 2) == 1
    late = lax.rem(col // 2, 2) == 1

    def turn(k):
        near, far = NEAR_FIRST[6], FAR_FIRST[6]
        for n in range(6):
            near = jnp.where(k == n, NEAR_FIRST[n], near)
            far = jnp.where(k == n, FAR_FIRST[n], far)
        d = jnp.where(late, far, near)
        return jnp.where(turned, 8 - d, d)

    @pl.loop(0, 7)
    def _(k):
        z_copy(turn(k)).start()

    qbuf[0] = dot32(normed, wqkv_v[0]).astype(BF16)

    loads[2].wait()
    gate = jax.nn.sigmoid(dot32(normed, wgate_v[...]))
    gsend[...] = gate.reshape(8, 8, 128)

    loads[3].wait()
    wb_t = wbias_v[...]
    ia = lax.broadcasted_iota(jnp.int32, (128, 128), 0)
    ib = lax.broadcasted_iota(jnp.int32, (128, 128), 1)
    centre = (jnp.where(ia == ib, 1.0, 0.0) - 1.0 / 128).astype(BF16)

    def bias_rows(n):
        pair_load(n).wait()
        c = dot32(pair_v[pl.ds(n * 8, 8)].reshape(2048, 128), centre)
        variance = jnp.mean(c * c, axis=1, keepdims=True)
        b = dot_nt(wb_t, (c * lax.rsqrt(variance + EPSILON)).astype(BF16)).astype(BF16).astype(F32)
        for i in range(8):
            for half in range(2):
                at = i * 256 + half * 128
                bias_v[half, pl.ds(n * 8 + i, 32, stride=64), :] = b[:, at : at + 128]

    def plane_copy(d, k):
        source = lax.rem(z + 8 - d, 8)
        return remote(
            zbuf.at[d], kv.at[lax.rem(source, 2) * 2 + core, col], a_s.at[d, k],
            kv_r.at[lax.rem(source, 2) * 2 + core, col], k * 16 + z * 2 + core, xh * 4 + source // 2,
        )

    def to_self(d, k):
        source = lax.rem(z + 8 - d, 8)
        return jnp.logical_and(xh == k, col == xh * 4 + source // 2)

    def forward(d):
        for k in range(2):
            here = to_self(d, k)

            @pl.when(here)
            def _():
                kv[lax.rem(z + 8 - d, 2) * 2 + core, col] = zbuf[d]

            @pl.when(jnp.logical_not(here))
            def _():
                plane_copy(d, k).start()

    forward(0)
    @pl.loop(1, 8)
    def _(d):
        q_copy(d).start()
        g_copy(d).start()

    @pl.loop(0, 8)
    def _(n):
        bias_rows(n)
        for half in range(2):
            k = n * 2 + half

            @pl.when(k < 7)
            def _():
                z_copy(turn(k)).wait_recv()
                forward(turn(k))

    def kv_wait(q, c):
        return remote(kv.at[q, c], kv.at[q, c], d_s.at[0, 0], kv_r.at[q, c], partner, col)

    def core_copy(h, c):
        q = h * 2 + core
        return remote(kv.at[q, c], kv.at[q, c], d_s.at[h, c], kv_r.at[q, c], partner, col)

    @pl.loop(0, 8)
    def _(d):
        c = lax.rem(col + 8 - d, 8)
        for h in range(2):
            @pl.when(jnp.logical_not(jnp.logical_and(own_plane, col == c)))
            def _():
                kv_wait(h * 2 + core, c).wait_recv()

            core_copy(h, c).start()

    @pl.loop(1, 8)
    def _(d):
        q_copy(d).wait_recv()


    ml_c[...] = jnp.zeros_like(ml_c)
    head_of = lane // 32

    @pl.loop(0, 8, unroll=4)
    def _(d):
        g = lax.rem(col + 8 - d, 8)
        for h in range(2):
            kv_wait(h * 2 + 1 - core, g).wait_recv()
        q = qbuf[d].astype(F32)
        q4 = jnp.concatenate([jnp.where(head_of == t, q, 0.0) for t in range(4)], axis=0).astype(BF16)
        blocks = [kv[b, g] for b in range(4)]
        keys = jnp.concatenate([b[0:64] for b in blocks], axis=0)
        values = jnp.concatenate([b[64:128] for b in blocks], axis=0)
        at = pl.ds(pl.multiple_of(g * 256, 256), 256)
        bias = jnp.concatenate([bias_v[0, at], bias_v[1, at]], axis=1)
        scores = dot_nt(q4, keys) * SCALE + bias
        peak = jnp.max(scores, axis=1, keepdims=True)
        weights = jnp.exp(scores - peak)
        total = jnp.sum(weights, axis=1, keepdims=True)
        o4 = dot32(weights.astype(BF16), values)
        out = jnp.zeros((64, 128), F32)
        ml = ml_c[...]
        for t in range(4):
            part = slice(t * 64, t * 64 + 64)
            out = jnp.where(head_of == t, o4[part], out)
            ml = jnp.where(lane == g * 4 + t, peak[part], jnp.where(lane == 32 + g * 4 + t, total[part], ml))
        ml_c[...] = ml
        o32[:, pl.ds(pl.multiple_of(g * 8, 8), 8), :] = out.reshape(8, 8, 128)

    osend[...] = o32[...].astype(BF16)
    mlsend[...] = ml_c[...].reshape(8, 8, 128)

    def o_copy(d):
        return col_copy(osend.at[lax.rem(col + d, 8)], orecv.at[d], o_s, o_r, d)

    def ml_copy(d):
        return col_copy(mlsend.at[lax.rem(col + d, 8)], mlrecv.at[d], ml_s, ml_r, d)

    @pl.loop(1, 8)
    def _(d):
        ml_copy(d).start()
        o_copy(d).start()

    orecv[0] = osend[col]
    mlrecv[0] = mlsend[col]
    grecv[0] = gsend[col]
    ea = lax.broadcasted_iota(jnp.int32, (128, 1024), 0)
    eb = lax.broadcasted_iota(jnp.int32, (128, 1024), 1)
    expand = jnp.where(ea == eb // 32, 1.0, 0.0).astype(BF16)
    @pl.loop(1, 8)
    def _(d):
        g_copy(d).wait_recv()
        ml_copy(d).wait_recv()
        o_copy(d).wait_recv()

    peaks = [mlrecv[p] for p in range(8)]
    sums = [pltpu.roll(v, 96, 1) for v in peaks]
    partials = [orecv[p].astype(F32) for p in range(8)]
    top = functools.reduce(jnp.maximum, peaks)
    shares = [jnp.exp(v - top) for v in peaks]
    whole = functools.reduce(jnp.add, [s * v for s, v in zip(shares, sums)])
    share = jnp.concatenate([jnp.where(lane < 32, s / whole, 0.0) for s in shares], axis=0)
    high = share.astype(BF16)
    low = (share - high.astype(F32)).astype(BF16)
    wide = dot32(high, expand) + dot32(low, expand)
    parts = []
    for g in range(8):
        tile = jnp.zeros((8, 128), F32)
        for p in range(8):
            tile = tile + wide[p * 8 : p * 8 + 8, g * 128 : g * 128 + 128] * partials[p][g * 8 : g * 8 + 8]
        parts.append(tile * grecv[lax.rem(col + 8 - g, 8)])
    attended = jnp.concatenate(parts, axis=1).astype(BF16)
    loads[4].wait()
    update = dot32(attended, wout_v[...])
    new_seq = (seq32[pl.ds(pl.multiple_of(col * 8, 8), 8), :] + update).astype(BF16).astype(F32)
    new_normed = norm_rows(new_seq).astype(BF16)
    loads[5].wait()
    sides = dot32(new_normed, wsp_v[...]).astype(BF16)
    lrsend[...] = sides

    def r_copy(n):
        return remote(lrsend, rbuf.at[lax.rem(row, 4), col], r_s.at[n], r_r.at[lax.rem(row, 4), col], n, row // 4)

    def l_copy(d):
        return remote(lrsend, lbuf.at[col], l_s.at[d], l_r.at[col], row, lax.rem(col + d, 8))

    def so_copy(d):
        return remote(sosend, sobuf.at[col], so_s.at[d], so_r.at[col], row, lax.rem(col + d, 8))

    def right_here(n):
        return jnp.logical_and(own_right, row == n)

    @pl.loop(0, 32)
    def _(j):
        far = j // 4
        far = 4 + (far + 1) // 2 * (1 - 2 * lax.rem(far, 2))
        n = lax.rem(j // 2, 2) * 16 + lax.rem(z + far, 8) * 2 + lax.rem(j, 2)

        @pl.when(jnp.logical_not(right_here(n)))
        def _():
            r_copy(n).start()

    @pl.loop(1, 8)
    def _(d):
        l_copy(d).start()

    sosend[...] = jnp.concatenate([new_seq[:, g * 128 : g * 128 + 128] for g in range(8)], axis=0).astype(BF16)

    @pl.loop(1, 8)
    def _(d):
        so_copy(d).start()

    own = [
        pltpu.make_async_copy(src, dst, own_sem.at[n])
        for n, (src, dst) in enumerate(
            ((lrsend, lbuf.at[col]), (sosend, sobuf.at[col]), (lrsend, rbuf.at[lax.rem(row, 4), col]))
        )
    ]
    own[0].start()
    own[1].start()

    @pl.when(own_right)
    def _():
        own[2].start()

    @pl.loop(1, 8)
    def _(d):
        z_copy(d).wait_send()
        q_copy(d).wait_send()
        g_copy(d).wait_send()
        ml_copy(d).wait_send()
        o_copy(d).wait_send()

    @pl.loop(0, 8)
    def _(d):
        for k in range(2):
            @pl.when(jnp.logical_not(to_self(d, k)))
            def _():
                plane_copy(d, k).wait_send()

    for h in range(2):
        @pl.loop(0, 8)
        def _(c):
            core_copy(h, c).wait_send()

    @pl.loop(1, 8)
    def _(d):
        l_copy(d).wait_send()
        so_copy(d).wait_send()

    @pl.loop(0, 32)
    def _(n):
        @pl.when(jnp.logical_not(right_here(n)))
        def _():
            r_copy(n).wait_send()

    own[0].wait()
    own[1].wait()

    @pl.when(own_right)
    def _():
        own[2].wait()

    def col_wait(buf, ss, rs, d):
        source = lax.rem(col + 8 - d, 8)
        return remote(buf.at[source], buf.at[source], ss.at[d], rs.at[source], row, source)

    @pl.loop(1, 8)
    def _(d):
        col_wait(lbuf, l_s, l_r, d).wait_recv()
        col_wait(sobuf, so_s, so_r, d).wait_recv()

    @pl.loop(0, 32)
    def _(n):
        q, c = n // 8, lax.rem(n, 8)

        @pl.when(jnp.logical_not(jnp.logical_and(own_right, jnp.logical_and(lax.rem(row, 4) == q, col == c))))
        def _():
            remote(rbuf.at[q, c], rbuf.at[q, c], r_s.at[0], r_r.at[q, c], partner, col).wait_recv()


def front(seq_state, pair_state, w_bias, w_qkv, w_gate, w_out, w_seq_pair):
    any_spec = pl.BlockSpec(memory_space=pl.ANY)
    dma = pltpu.SemaphoreType.DMA
    return pl.pallas_call(
        front_kernel,
        out_shape=(
            jax.ShapeDtypeStruct((8, 64, 128), BF16),
            jax.ShapeDtypeStruct((8, 8, 128), BF16),
            jax.ShapeDtypeStruct((4, 8, 8, 128), BF16),
        ),
        in_specs=[any_spec] * 7,
        out_specs=(any_spec,) * 3,
        scratch_shapes=[
            pltpu.VMEM((64, 1024), BF16),
            pltpu.VMEM((64, 256, 128), BF16),
            pltpu.VMEM((32, 128), BF16),
            pltpu.VMEM((3, 1024, 128), BF16),
            pltpu.VMEM((1024, 128), BF16),
            pltpu.VMEM((1024, 1024), BF16),
            pltpu.VMEM((1024, 128), BF16),
            pltpu.VMEM((64, 1024), F32),
            pltpu.VMEM((8, 128, 128), BF16),
            pltpu.VMEM((8, 64, 128), BF16),
            pltpu.VMEM((8, 8, 128), F32),
            pltpu.VMEM((8, 8, 128), F32),
            pltpu.VMEM((4, 8, 128, 128), BF16),
            pltpu.VMEM((2, 2048, 128), F32),
            pltpu.VMEM((8, 64, 128), F32),
            pltpu.VMEM((8, 64, 128), BF16),
            pltpu.VMEM((8, 64, 128), BF16),
            pltpu.VMEM((64, 128), F32),
            pltpu.VMEM((8, 8, 128), F32),
            pltpu.VMEM((8, 8, 128), F32),
            pltpu.VMEM((8, 128), BF16),
            pltpu.VMEM((64, 128), BF16),
            dma((6,)), dma((8,)), dma((3,)),
            dma((8,)), dma((8,)), dma((8,)), dma((8,)), dma((8,)), dma((8,)),
            dma((8, 2)), dma((4, 8)), dma((2, 8)),
            dma((8,)), dma((8,)), dma((8,)), dma((8,)), dma((8,)), dma((8,)),
            dma((32,)), dma((4, 8)), dma((8,)), dma((8,)),
        ],
        compiler_params=pltpu.CompilerParams(
            collective_id=0, has_side_effects=True, vmem_limit_bytes=67_043_328
        ),
        cost_estimate=pl.CostEstimate(flops=3_000_000_000, bytes_accessed=8_000_000, transcendentals=600_000),
    )(seq_state, pair_state, w_bias, w_qkv, w_gate, w_out, w_seq_pair)


def pair_kernel(x_ref, left_ref, right_ref, wp_ref, wu_ref, wd_ref, seq_ref, o_ref, seq_out_ref, mix_ref, right2_ref):
    @pl.when(pl.program_id(0) == 0)
    def _():
        w = wp_ref[...].astype(F32)
        centred = w - jnp.mean(w, axis=1, keepdims=True)
        a = lax.broadcasted_iota(jnp.int32, (128, 128), 0)
        b = lax.broadcasted_iota(jnp.int32, (128, 128), 1)
        eye = jnp.where(a == b, 1.0, 0.0)
        mix_ref[0:128, 0:128] = (eye - 1.0 / 128).astype(BF16)
        mix_ref[0:128, 128:256] = eye.astype(BF16)
        mix_ref[128:256, 0:128] = centred.astype(BF16)
        mix_ref[128:256, 128:256] = wp_ref[...]
        r = right_ref[...].astype(F32).reshape(256, 128)[:, 64:128]
        right2_ref[...] = jnp.concatenate([r, r], axis=1).astype(BF16)
        rows = seq_ref[...].astype(F32)
        seq_out_ref[...] = jnp.concatenate(
            [rows[:, g * 8 : g * 8 + 8, :].reshape(64, 128) for g in range(8)], axis=1
        ).astype(BF16)

    lane = lax.broadcasted_iota(jnp.int32, (1, 128), 1)

    lefts = left_ref[...].astype(F32).reshape(PAIR_ROWS, 128)

    def update(start):
        features, rows = [], []
        for i in range(start, start + PAIR_CHUNK):
            left = lefts[i : i + 1, 0:64]
            left2 = jnp.concatenate([left, left], axis=1)
            scale = jnp.where(lane < 64, left2, -1.0).astype(BF16)
            shift = jnp.where(lane < 64, 0.0, left2).astype(BF16)
            features.append(right2_ref[...] * scale + shift)
            rows.append(x_ref[i])
        mixed = dot32(
            jnp.concatenate([jnp.concatenate(rows, axis=0), jnp.concatenate(features, axis=0)], axis=1),
            mix_ref[...],
        )
        return mixed[:, :128], mixed[:, 128:]

    def normed(centred):
        variance = jnp.mean(centred * centred, axis=1, keepdims=True)
        return (centred * lax.rsqrt(variance + EPSILON)).astype(BF16)

    def finish(start, hidden, updated):
        result = (updated + dot32(hidden, wd_ref[...])).astype(BF16)
        for i in range(PAIR_CHUNK):
            o_ref[start + i] = result[i * 256 : (i + 1) * 256]

    count = PAIR_ROWS // PAIR_CHUNK
    ready, updates, hidden = {}, {}, {}
    for t in range(count + 2):
        if t < count:
            centred, updates[t] = update(t * PAIR_CHUNK)
        if 0 <= t - 1 < count:
            hidden[t - 1] = jnp.maximum(dot32(ready[t - 1], wu_ref[...]).astype(BF16), 0)
        if t < count:
            ready[t] = normed(centred)
        if 0 <= t - 2:
            finish((t - 2) * PAIR_CHUNK, hidden[t - 2], updates[t - 2])


def pair_transition(x, left, right, wp, wu, wd, seq):
    rows = x.shape[0]

    def whole(shape):
        return pl.BlockSpec(shape, lambda i: (0,) * len(shape))

    return pl.pallas_call(
        pair_kernel,
        grid=(rows // PAIR_ROWS,),
        out_shape=(jax.ShapeDtypeStruct(x.shape, BF16), jax.ShapeDtypeStruct((64, 1024), BF16)),
        in_specs=[
            pl.BlockSpec((PAIR_ROWS, 256, 128), lambda i: (i, 0, 0)),
            pl.BlockSpec((PAIR_ROWS // 8, 8, 128), lambda i: (i, 0, 0)),
            whole(right.shape),
            whole(wp.shape),
            whole(wu.shape),
            whole(wd.shape),
            whole(seq.shape),
        ],
        out_specs=(pl.BlockSpec((PAIR_ROWS, 256, 128), lambda i: (i, 0, 0)), whole((64, 1024))),
        scratch_shapes=[pltpu.VMEM((256, 256), BF16), pltpu.VMEM((256, 128), BF16)],
        compiler_params=pltpu.CompilerParams(dimension_semantics=("arbitrary",)),
    )(x, left, right, wp, wu, wd, seq)


def body(seq_state, pair_state, w_bias, w_qkv, w_gate, w_out, w_seq_pair, w_pair_out, w_up, w_down):
    seq_rows, left, right = front(seq_state, pair_state, w_bias.T, w_qkv, w_gate, w_out, w_seq_pair)
    pair_out, seq_out = pair_transition(pair_state, left, right, w_pair_out, w_up, w_down, seq_rows)
    return (seq_out, pair_out)


def solution(mesh):
    return jax.shard_map(
        body,
        mesh=mesh,
        in_specs=(
            P("row", None),
            P("row", "col", None),
            P(),
            P(None, None, "col"),
            P(None, "col"),
            P(),
            P(),
            P(),
            P(),
            P(),
        ),
        out_specs=(P("row", None), P("row", "col", None)),
        check_vma=False,
    )
```

```python
import functools
import math

import jax
import jax.numpy as jnp
from jax import lax
from jax.experimental import pallas as pl
from jax.experimental.pallas import tpu as pltpu
from jax.sharding import PartitionSpec as P

EPSILON = 1e-05
F32 = jnp.float32
BF16 = jnp.bfloat16
PAIR_ROWS = 16
PAIR_CHUNK = 4
SCALE = 1.0 / math.sqrt(32)
NT = (((1,), (1,)), ((), ()))
NEAR_FIRST = (1, 7, 2, 6, 3, 5, 4)
FAR_FIRST = (3, 5, 4, 2, 1, 7, 6)


def dot32(a, b):
    return jnp.dot(a, b, preferred_element_type=F32)


def dot_nt(a, b):
    return lax.dot_general(a, b, NT, preferred_element_type=F32)


def norm_rows(values):
    centred = values - jnp.mean(values, axis=-1, keepdims=True)
    variance = jnp.mean(centred * centred, axis=-1, keepdims=True)
    return centred * lax.rsqrt(variance + EPSILON)


def front_kernel(
    seq_hbm, pair_hbm, wbias_hbm, wqkv_hbm, wgate_hbm, wout_hbm, wsp_hbm,
    sobuf, lbuf, rbuf,
    seq_v, pair_v, wbias_v, wqkv_v, wgate_v, wout_v, wsp_v,
    seq32, zbuf, qbuf, gsend, grecv, kv, bias_v, o32, osend, orecv, ml_c, mlsend, mlrecv,
    lrsend, sosend,
    in_sem, pair_sem, own_sem,
    z_s, z_r, q_s, q_r, g_s, g_r, a_s, kv_r, d_s, o_s, o_r, ml_s, ml_r, l_s, l_r, r_s, r_r, so_s, so_r,
):
    row = lax.axis_index("row")
    col = lax.axis_index("col")
    core = lax.rem(row, 2)
    z = lax.rem(row // 2, 8)
    xh = row // 16
    partner = row + 1 - 2 * core
    own_plane = xh == col // 4
    own_right = row // 4 == col

    loads = [
        pltpu.make_async_copy(src, dst, in_sem.at[n])
        for n, (src, dst) in enumerate(
            ((seq_hbm, seq_v), (wqkv_hbm.at[pl.ds(1, 2)], wqkv_v.at[pl.ds(1, 2)]), (wgate_hbm, wgate_v),
             (wbias_hbm, wbias_v), (wout_hbm, wout_v), (wsp_hbm, wsp_v), (wqkv_hbm.at[0], wqkv_v.at[0]))
        )
    ]
    for n in (0, 1, 6, 2, 3):
        loads[n].start()

    barrier = pltpu.get_barrier_semaphore()

    def greet(r, c):
        pl.semaphore_signal(barrier, inc=1, device_id=(r, c), device_id_type=pl.DeviceIdType.MESH)

    def z_row(k):
        return xh * 16 + lax.rem(z + k, 8) * 2 + core

    for d in range(1, 8):
        greet(z_row(d), col)
        greet(row, lax.rem(col + d, 8))
    greet(partner, col)
    plane_row = (col // 4) * 16 + z * 2 + core
    for c in range(8):
        @pl.when(jnp.logical_not(jnp.logical_and(own_plane, col == c)))
        def _():
            greet(plane_row, c)

    def pair_load(n):
        return pltpu.make_async_copy(pair_hbm.at[pl.ds(n * 8, 8)], pair_v.at[pl.ds(n * 8, 8)], pair_sem.at[n])

    lane = lax.broadcasted_iota(jnp.int32, (1, 128), 1)
    loads[0].wait()
    x = seq_v[...].astype(F32)
    seq32[...] = x
    normed = norm_rows(x).astype(BF16)
    loads[1].wait()
    for n in range(8):
        pair_load(n).start()
    for n in (4, 5):
        loads[n].start()
    zbuf[0, 0:64] = dot32(normed, wqkv_v[1]).astype(BF16)
    zbuf[0, 64:128] = dot32(normed, wqkv_v[2]).astype(BF16)

    pl.semaphore_wait(barrier, 15 + 8 - own_plane.astype(jnp.int32))

    def remote(src, dst, ss, rs, r, c):
        return pltpu.make_async_remote_copy(
            src_ref=src, dst_ref=dst, send_sem=ss, recv_sem=rs, device_id=(r, c),
            device_id_type=pl.DeviceIdType.MESH,
        )

    def z_copy(d):
        return remote(zbuf.at[0], zbuf.at[d], z_s.at[d], z_r.at[d], z_row(d), col)

    def col_copy(src, dst, ss, rs, d):
        return remote(src, dst, ss.at[d], rs.at[d], row, lax.rem(col + d, 8))

    def q_copy(d):
        return col_copy(qbuf.at[0], qbuf.at[d], q_s, q_r, d)

    def g_copy(d):
        return col_copy(gsend.at[lax.rem(col + d, 8)], grecv.at[d], g_s, g_r, d)

    turned = lax.rem(col, 2) == 1
    late = lax.rem(col // 2, 2) == 1

    def turn(k):
        near, far = NEAR_FIRST[6], FAR_FIRST[6]
        for n in range(6):
            near = jnp.where(k == n, NEAR_FIRST[n], near)
            far = jnp.where(k == n, FAR_FIRST[n], far)
        d = jnp.where(late, far, near)
        return jnp.where(turned, 8 - d, d)

    @pl.loop(0, 7)
    def _(k):
        z_copy(turn(k)).start()


    loads[3].wait()
    wb_t = wbias_v[...]
    ia = lax.broadcasted_iota(jnp.int32, (128, 128), 0)
    ib = lax.broadcasted_iota(jnp.int32, (128, 128), 1)
    centre = (jnp.where(ia == ib, 1.0, 0.0) - 1.0 / 128).astype(BF16)

    def bias_rows(n):
        pair_load(n).wait()
        c = dot32(pair_v[pl.ds(n * 8, 8)].reshape(2048, 128), centre)
        variance = jnp.mean(c * c, axis=1, keepdims=True)
        b = dot_nt(wb_t, (c * lax.rsqrt(variance + EPSILON)).astype(BF16)).astype(BF16).astype(F32)
        for i in range(8):
            for half in range(2):
                at = i * 256 + half * 128
                bias_v[half, pl.ds(n * 8 + i, 32, stride=64), :] = b[:, at : at + 128]

    def plane_copy(d, k):
        source = lax.rem(z + 8 - d, 8)
        return remote(
            zbuf.at[d], kv.at[lax.rem(source, 2) * 2 + core, col], a_s.at[d, k],
            kv_r.at[lax.rem(source, 2) * 2 + core, col], k * 16 + z * 2 + core, xh * 4 + source // 2,
        )

    def to_self(d, k):
        source = lax.rem(z + 8 - d, 8)
        return jnp.logical_and(xh == k, col == xh * 4 + source // 2)

    def forward(d):
        for k in range(2):
            here = to_self(d, k)

            @pl.when(here)
            def _():
                kv[lax.rem(z + 8 - d, 2) * 2 + core, col] = zbuf[d]

            @pl.when(jnp.logical_not(here))
            def _():
                plane_copy(d, k).start()

    forward(0)
    loads[6].wait()
    qbuf[0] = dot32(normed, wqkv_v[0]).astype(BF16)

    @pl.loop(1, 8)
    def _(d):
        q_copy(d).start()

    loads[2].wait()
    gate = jax.nn.sigmoid(dot32(normed, wgate_v[...]))
    gsend[...] = gate.reshape(8, 8, 128)

    @pl.loop(1, 8)
    def _(d):
        g_copy(d).start()

    @pl.loop(0, 8)
    def _(n):
        bias_rows(n)
        for half in range(2):
            k = n * 2 + half

            @pl.when(k < 7)
            def _():
                z_copy(turn(k)).wait_recv()
                forward(turn(k))

    def kv_wait(q, c):
        return remote(kv.at[q, c], kv.at[q, c], d_s.at[0, 0], kv_r.at[q, c], partner, col)

    def core_copy(h, c):
        q = h * 2 + core
        return remote(kv.at[q, c], kv.at[q, c], d_s.at[h, c], kv_r.at[q, c], partner, col)

    @pl.loop(0, 8)
    def _(d):
        c = lax.rem(col + 8 - d, 8)
        for h in range(2):
            @pl.when(jnp.logical_not(jnp.logical_and(own_plane, col == c)))
            def _():
                kv_wait(h * 2 + core, c).wait_recv()

            core_copy(h, c).start()

    @pl.loop(1, 8)
    def _(d):
        q_copy(d).wait_recv()


    ml_c[...] = jnp.zeros_like(ml_c)
    head_of = lane // 32

    @pl.loop(0, 8, unroll=4)
    def _(d):
        g = lax.rem(col + 8 - d, 8)
        for h in range(2):
            kv_wait(h * 2 + 1 - core, g).wait_recv()
        q = qbuf[d].astype(F32)
        q4 = jnp.concatenate([jnp.where(head_of == t, q, 0.0) for t in range(4)], axis=0).astype(BF16)
        blocks = [kv[b, g] for b in range(4)]
        keys = jnp.concatenate([b[0:64] for b in blocks], axis=0)
        values = jnp.concatenate([b[64:128] for b in blocks], axis=0)
        at = pl.ds(pl.multiple_of(g * 256, 256), 256)
        bias = jnp.concatenate([bias_v[0, at], bias_v[1, at]], axis=1)
        scores = dot_nt(q4, keys) * SCALE + bias
        peak = jnp.max(scores, axis=1, keepdims=True)
        weights = jnp.exp(scores - peak)
        total = jnp.sum(weights, axis=1, keepdims=True)
        o4 = dot32(weights.astype(BF16), values)
        out = jnp.zeros((64, 128), F32)
        ml = ml_c[...]
        for t in range(4):
            part = slice(t * 64, t * 64 + 64)
            out = jnp.where(head_of == t, o4[part], out)
            ml = jnp.where(lane == g * 4 + t, peak[part], jnp.where(lane == 32 + g * 4 + t, total[part], ml))
        ml_c[...] = ml
        o32[:, pl.ds(pl.multiple_of(g * 8, 8), 8), :] = out.reshape(8, 8, 128)

    osend[...] = o32[...].astype(BF16)
    mlsend[...] = ml_c[...].reshape(8, 8, 128)

    def o_copy(d):
        return col_copy(osend.at[lax.rem(col + d, 8)], orecv.at[d], o_s, o_r, d)

    def ml_copy(d):
        return col_copy(mlsend.at[lax.rem(col + d, 8)], mlrecv.at[d], ml_s, ml_r, d)

    @pl.loop(1, 8)
    def _(d):
        ml_copy(d).start()
        o_copy(d).start()

    orecv[0] = osend[col]
    mlrecv[0] = mlsend[col]
    grecv[0] = gsend[col]
    ea = lax.broadcasted_iota(jnp.int32, (128, 1024), 0)
    eb = lax.broadcasted_iota(jnp.int32, (128, 1024), 1)
    expand = jnp.where(ea == eb // 32, 1.0, 0.0).astype(BF16)
    @pl.loop(1, 8)
    def _(d):
        g_copy(d).wait_recv()
        ml_copy(d).wait_recv()
        o_copy(d).wait_recv()

    peaks = [mlrecv[p] for p in range(8)]
    sums = [pltpu.roll(v, 96, 1) for v in peaks]
    partials = [orecv[p].astype(F32) for p in range(8)]
    top = functools.reduce(jnp.maximum, peaks)
    shares = [jnp.exp(v - top) for v in peaks]
    whole = functools.reduce(jnp.add, [s * v for s, v in zip(shares, sums)])
    share = jnp.concatenate([jnp.where(lane < 32, s / whole, 0.0) for s in shares], axis=0)
    high = share.astype(BF16)
    low = (share - high.astype(F32)).astype(BF16)
    wide = dot32(high, expand) + dot32(low, expand)
    parts = []
    for g in range(8):
        tile = jnp.zeros((8, 128), F32)
        for p in range(8):
            tile = tile + wide[p * 8 : p * 8 + 8, g * 128 : g * 128 + 128] * partials[p][g * 8 : g * 8 + 8]
        parts.append(tile * grecv[lax.rem(col + 8 - g, 8)])
    attended = jnp.concatenate(parts, axis=1).astype(BF16)
    loads[4].wait()
    update = dot32(attended, wout_v[...])
    new_seq = (seq32[pl.ds(pl.multiple_of(col * 8, 8), 8), :] + update).astype(BF16).astype(F32)
    new_normed = norm_rows(new_seq).astype(BF16)
    loads[5].wait()
    sides = dot32(new_normed, wsp_v[...]).astype(BF16)
    lrsend[...] = sides

    def r_copy(n):
        return remote(lrsend, rbuf.at[lax.rem(row, 4), col], r_s.at[n], r_r.at[lax.rem(row, 4), col], n, row // 4)

    def l_copy(d):
        return remote(lrsend, lbuf.at[col], l_s.at[d], l_r.at[col], row, lax.rem(col + d, 8))

    def so_copy(d):
        return remote(sosend, sobuf.at[col], so_s.at[d], so_r.at[col], row, lax.rem(col + d, 8))

    def right_here(n):
        return jnp.logical_and(own_right, row == n)

    @pl.loop(0, 32)
    def _(j):
        far = j // 4
        far = 4 + (far + 1) // 2 * (1 - 2 * lax.rem(far, 2))
        n = lax.rem(j // 2, 2) * 16 + lax.rem(z + far, 8) * 2 + lax.rem(j, 2)

        @pl.when(jnp.logical_not(right_here(n)))
        def _():
            r_copy(n).start()

    @pl.loop(1, 8)
    def _(d):
        l_copy(d).start()

    sosend[...] = jnp.concatenate([new_seq[:, g * 128 : g * 128 + 128] for g in range(8)], axis=0).astype(BF16)

    @pl.loop(1, 8)
    def _(d):
        so_copy(d).start()

    own = [
        pltpu.make_async_copy(src, dst, own_sem.at[n])
        for n, (src, dst) in enumerate(
            ((lrsend, lbuf.at[col]), (sosend, sobuf.at[col]), (lrsend, rbuf.at[lax.rem(row, 4), col]))
        )
    ]
    own[0].start()
    own[1].start()

    @pl.when(own_right)
    def _():
        own[2].start()

    @pl.loop(1, 8)
    def _(d):
        z_copy(d).wait_send()
        q_copy(d).wait_send()
        g_copy(d).wait_send()
        ml_copy(d).wait_send()
        o_copy(d).wait_send()

    @pl.loop(0, 8)
    def _(d):
        for k in range(2):
            @pl.when(jnp.logical_not(to_self(d, k)))
            def _():
                plane_copy(d, k).wait_send()

    for h in range(2):
        @pl.loop(0, 8)
        def _(c):
            core_copy(h, c).wait_send()

    @pl.loop(1, 8)
    def _(d):
        l_copy(d).wait_send()
        so_copy(d).wait_send()

    @pl.loop(0, 32)
    def _(n):
        @pl.when(jnp.logical_not(right_here(n)))
        def _():
            r_copy(n).wait_send()

    own[0].wait()
    own[1].wait()

    @pl.when(own_right)
    def _():
        own[2].wait()

    def col_wait(buf, ss, rs, d):
        source = lax.rem(col + 8 - d, 8)
        return remote(buf.at[source], buf.at[source], ss.at[d], rs.at[source], row, source)

    @pl.loop(1, 8)
    def _(d):
        col_wait(lbuf, l_s, l_r, d).wait_recv()
        col_wait(sobuf, so_s, so_r, d).wait_recv()

    @pl.loop(0, 32)
    def _(n):
        q, c = n // 8, lax.rem(n, 8)

        @pl.when(jnp.logical_not(jnp.logical_and(own_right, jnp.logical_and(lax.rem(row, 4) == q, col == c))))
        def _():
            remote(rbuf.at[q, c], rbuf.at[q, c], r_s.at[0], r_r.at[q, c], partner, col).wait_recv()


def front(seq_state, pair_state, w_bias, w_qkv, w_gate, w_out, w_seq_pair):
    any_spec = pl.BlockSpec(memory_space=pl.ANY)
    dma = pltpu.SemaphoreType.DMA
    return pl.pallas_call(
        front_kernel,
        out_shape=(
            jax.ShapeDtypeStruct((8, 64, 128), BF16),
            jax.ShapeDtypeStruct((8, 8, 128), BF16),
            jax.ShapeDtypeStruct((4, 8, 8, 128), BF16),
        ),
        in_specs=[any_spec] * 7,
        out_specs=(any_spec,) * 3,
        scratch_shapes=[
            pltpu.VMEM((64, 1024), BF16),
            pltpu.VMEM((64, 256, 128), BF16),
            pltpu.VMEM((32, 128), BF16),
            pltpu.VMEM((3, 1024, 128), BF16),
            pltpu.VMEM((1024, 128), BF16),
            pltpu.VMEM((1024, 1024), BF16),
            pltpu.VMEM((1024, 128), BF16),
            pltpu.VMEM((64, 1024), F32),
            pltpu.VMEM((8, 128, 128), BF16),
            pltpu.VMEM((8, 64, 128), BF16),
            pltpu.VMEM((8, 8, 128), F32),
            pltpu.VMEM((8, 8, 128), F32),
            pltpu.VMEM((4, 8, 128, 128), BF16),
            pltpu.VMEM((2, 2048, 128), F32),
            pltpu.VMEM((8, 64, 128), F32),
            pltpu.VMEM((8, 64, 128), BF16),
            pltpu.VMEM((8, 64, 128), BF16),
            pltpu.VMEM((64, 128), F32),
            pltpu.VMEM((8, 8, 128), F32),
            pltpu.VMEM((8, 8, 128), F32),
            pltpu.VMEM((8, 128), BF16),
            pltpu.VMEM((64, 128), BF16),
            dma((7,)), dma((8,)), dma((3,)),
            dma((8,)), dma((8,)), dma((8,)), dma((8,)), dma((8,)), dma((8,)),
            dma((8, 2)), dma((4, 8)), dma((2, 8)),
            dma((8,)), dma((8,)), dma((8,)), dma((8,)), dma((8,)), dma((8,)),
            dma((32,)), dma((4, 8)), dma((8,)), dma((8,)),
        ],
        compiler_params=pltpu.CompilerParams(
            collective_id=0, has_side_effects=True, vmem_limit_bytes=67_043_328
        ),
        cost_estimate=pl.CostEstimate(flops=3_000_000_000, bytes_accessed=8_000_000, transcendentals=600_000),
    )(seq_state, pair_state, w_bias, w_qkv, w_gate, w_out, w_seq_pair)


def pair_kernel(x_ref, left_ref, right_ref, wp_ref, wu_ref, wd_ref, seq_ref, o_ref, seq_out_ref, mix_ref, right2_ref):
    @pl.when(pl.program_id(0) == 0)
    def _():
        w = wp_ref[...].astype(F32)
        centred = w - jnp.mean(w, axis=1, keepdims=True)
        a = lax.broadcasted_iota(jnp.int32, (128, 128), 0)
        b = lax.broadcasted_iota(jnp.int32, (128, 128), 1)
        eye = jnp.where(a == b, 1.0, 0.0)
        mix_ref[0:128, 0:128] = (eye - 1.0 / 128).astype(BF16)
        mix_ref[0:128, 128:256] = eye.astype(BF16)
        mix_ref[128:256, 0:128] = centred.astype(BF16)
        mix_ref[128:256, 128:256] = wp_ref[...]
        r = right_ref[...].astype(F32).reshape(256, 128)[:, 64:128]
        right2_ref[...] = jnp.concatenate([r, r], axis=1).astype(BF16)

    lane = lax.broadcasted_iota(jnp.int32, (1, 128), 1)

    seq = seq_ref[...].astype(F32)
    seq_out_ref[...] = jnp.concatenate(
        [seq[:, g * 8 : g * 8 + 8, :].reshape(PAIR_ROWS, 128) for g in range(8)], axis=1
    ).astype(BF16)
    lefts = left_ref[...].astype(F32).reshape(PAIR_ROWS, 128)

    def update(start):
        features, rows = [], []
        for i in range(start, start + PAIR_CHUNK):
            left = lefts[i : i + 1, 0:64]
            left2 = jnp.concatenate([left, left], axis=1)
            scale = jnp.where(lane < 64, left2, -1.0).astype(BF16)
            shift = jnp.where(lane < 64, 0.0, left2).astype(BF16)
            features.append(right2_ref[...] * scale + shift)
            rows.append(x_ref[i])
        mixed = dot32(
            jnp.concatenate([jnp.concatenate(rows, axis=0), jnp.concatenate(features, axis=0)], axis=1),
            mix_ref[...],
        )
        return mixed[:, :128], mixed[:, 128:]

    def normed(centred):
        variance = jnp.mean(centred * centred, axis=1, keepdims=True)
        return (centred * lax.rsqrt(variance + EPSILON)).astype(BF16)

    def finish(start, hidden, updated):
        result = (updated + dot32(hidden, wd_ref[...])).astype(BF16)
        for i in range(PAIR_CHUNK):
            o_ref[start + i] = result[i * 256 : (i + 1) * 256]

    count = PAIR_ROWS // PAIR_CHUNK
    ready, updates, hidden = {}, {}, {}
    for t in range(count + 2):
        if t < count:
            centred, updates[t] = update(t * PAIR_CHUNK)
        if 0 <= t - 1 < count:
            hidden[t - 1] = jnp.maximum(dot32(ready[t - 1], wu_ref[...]).astype(BF16), 0)
        if t < count:
            ready[t] = normed(centred)
        if 0 <= t - 2:
            finish((t - 2) * PAIR_CHUNK, hidden[t - 2], updates[t - 2])


def pair_transition(x, left, right, wp, wu, wd, seq):
    rows = x.shape[0]

    def whole(shape):
        return pl.BlockSpec(shape, lambda i: (0,) * len(shape))

    return pl.pallas_call(
        pair_kernel,
        grid=(rows // PAIR_ROWS,),
        out_shape=(jax.ShapeDtypeStruct(x.shape, BF16), jax.ShapeDtypeStruct((64, 1024), BF16)),
        in_specs=[
            pl.BlockSpec((PAIR_ROWS, 256, 128), lambda i: (i, 0, 0)),
            pl.BlockSpec((PAIR_ROWS // 8, 8, 128), lambda i: (i, 0, 0)),
            whole(right.shape),
            whole(wp.shape),
            whole(wu.shape),
            whole(wd.shape),
            pl.BlockSpec((PAIR_ROWS // 8, 64, 128), lambda i: (i, 0, 0)),
        ],
        out_specs=(pl.BlockSpec((PAIR_ROWS, 256, 128), lambda i: (i, 0, 0)), pl.BlockSpec((PAIR_ROWS, 1024), lambda i: (i, 0))),
        scratch_shapes=[pltpu.VMEM((256, 256), BF16), pltpu.VMEM((256, 128), BF16)],
        compiler_params=pltpu.CompilerParams(dimension_semantics=("arbitrary",)),
    )(x, left, right, wp, wu, wd, seq)


def body(seq_state, pair_state, w_bias, w_qkv, w_gate, w_out, w_seq_pair, w_pair_out, w_up, w_down):
    seq_rows, left, right = front(seq_state, pair_state, w_bias.T, w_qkv, w_gate, w_out, w_seq_pair)
    pair_out, seq_out = pair_transition(pair_state, left, right, w_pair_out, w_up, w_down, seq_rows)
    return (seq_out, pair_out)


def solution(mesh):
    return jax.shard_map(
        body,
        mesh=mesh,
        in_specs=(
            P("row", None),
            P("row", "col", None),
            P(),
            P(None, None, "col"),
            P(None, "col"),
            P(),
            P(),
            P(),
            P(),
            P(),
        ),
        out_specs=(P("row", None), P("row", "col", None)),
        check_vma=False,
    )
```
